16 devices in a mesh: cp: 16 (over z, y, x, core).
Axes of the slice: x: 2, y: 2, z: 2, core: 2. Of those that a mesh axis runs over, the one named last changes fastest.
Arguments:
- queries: bfloat16 [1024, 128, 192], P('cp')
- latent: bfloat16 [1024, 512], P('cp')
- key_rope: bfloat16 [1024, 64], P('cp')
- w_uk: bfloat16 [512, 128, 128], replicated
- w_uv: bfloat16 [512, 128, 128], replicated
- d_out: bfloat16 [1024, 128, 128], P('cp')
Outputs:
- output 1: bfloat16 [1024, 128, 128], P('cp')
- output 2: bfloat16 [1024, 128, 192], P('cp')
- output 3: bfloat16 [1024, 512], P('cp')
- output 4: bfloat16 [1024, 64], P('cp')
- output 5: float32 [512, 128, 128], replicated
- output 6: float32 [512, 128, 128], replicated
All inputs are finite; a program needn't handle non-finite values.
Results may differ from the reference program's by a relative error of at most 0.0167186.
Values are sent between devices in bfloat16 or wider.
A program may use at most 1 GiB of HBM per device.

```python
import math
import jax
import jax.numpy as jnp
from jax import lax

TOK_DEV = 64
N_DEV = 16
N_HEADS = 128
LATENT = 512
NOPE_DIM = 128
ROPE_DIM = 64
V_DIM = 128

SEQ_LEN = TOK_DEV * N_DEV
QK_DIM = NOPE_DIM + ROPE_DIM
SOFT_SCALE = 1.0 / math.sqrt(QK_DIM)
Q_SPREAD = math.sqrt(0.75 * math.log(SEQ_LEN))


def setup_inputs(seed: int = 0) -> dict:
    rng_keys = jax.random.split(jax.random.key(seed), 6)
    queries = jax.random.normal(rng_keys[0], (SEQ_LEN, N_HEADS, QK_DIM), jnp.float32) * Q_SPREAD
    latent = jax.random.normal(rng_keys[1], (SEQ_LEN, LATENT), jnp.float32)
    key_rope = jax.random.normal(rng_keys[2], (SEQ_LEN, ROPE_DIM), jnp.float32)
    w_uk = jax.random.normal(rng_keys[3], (LATENT, N_HEADS, NOPE_DIM), jnp.float32) * LATENT ** -0.5
    w_uv = jax.random.normal(rng_keys[4], (LATENT, N_HEADS, V_DIM), jnp.float32) * LATENT ** -0.5
    d_out = jax.random.normal(rng_keys[5], (SEQ_LEN, N_HEADS, V_DIM), jnp.float32)
    return {
        "queries": queries.astype(jnp.bfloat16),
        "latent": latent.astype(jnp.bfloat16),
        "key_rope": key_rope.astype(jnp.bfloat16),
        "w_uk": w_uk.astype(jnp.bfloat16),
        "w_uv": w_uv.astype(jnp.bfloat16),
        "d_out": d_out.astype(jnp.bfloat16),
    }


def decompress(latent, w_uk, w_uv):
    lat_f = latent.astype(jnp.float32)
    k_nope = jnp.einsum("tl,lhd->thd", lat_f, w_uk.astype(jnp.float32)).astype(jnp.bfloat16)
    values = jnp.einsum("tl,lhd->thd", lat_f, w_uv.astype(jnp.float32)).astype(jnp.bfloat16)
    return k_nope, values


def attend(queries, latent, key_rope, w_uk, w_uv):
    k_nope, values = decompress(latent, w_uk, w_uv)
    k_f = k_nope.astype(jnp.float32)
    v_f = values.astype(jnp.float32)
    r_f = key_rope.astype(jnp.float32)
    key_pos = jnp.arange(SEQ_LEN)

    def block_rows(blk_pair):
        q_blk, q_start = blk_pair
        q_f = q_blk.astype(jnp.float32)
        scores = (jnp.einsum("qhd,khd->hqk", q_f[:, :, :NOPE_DIM], k_f)
                  + jnp.einsum("qhd,kd->hqk", q_f[:, :, NOPE_DIM:], r_f)) * SOFT_SCALE
        q_pos = q_start + jnp.arange(TOK_DEV)
        visible = key_pos[None, :] <= q_pos[:, None]
        scores = jnp.where(visible[None], scores, -1e30)
        attn_prob = jax.nn.softmax(scores, axis=-1)
        return jnp.einsum("hqk,khd->qhd", attn_prob, v_f)

    q_blocks = queries.reshape(N_DEV, TOK_DEV, N_HEADS, QK_DIM)
    q_starts = jnp.arange(N_DEV) * TOK_DEV
    out_rows = lax.map(jax.checkpoint(block_rows), (q_blocks, q_starts))
    return out_rows.reshape(SEQ_LEN, N_HEADS, V_DIM).astype(jnp.bfloat16)


def reference(queries, latent, key_rope, w_uk, w_uv, d_out):
    attn_out, pull_back = jax.vjp(attend, queries, latent, key_rope, w_uk.astype(jnp.float32), w_uv.astype(jnp.float32))
    d_query, d_latent, d_key_rope, d_w_uk, d_w_uv = pull_back(d_out)
    return (attn_out, d_query.astype(jnp.bfloat16), d_latent.astype(jnp.bfloat16), d_key_rope.astype(jnp.bfloat16), d_w_uk, d_w_uv)
```

```python
import functools
import math
import jax
import jax.numpy as jnp
from jax import lax
from jax.experimental import pallas as pl
from jax.experimental.pallas import tpu as pltpu
from jax.sharding import PartitionSpec as P

N_CHUNK = 4
Q_BLK = 256
LOG2E = 1.4426950408889634
F32 = jnp.float32
BF16 = jnp.bfloat16


def dot(a, b):
    return lax.dot_general(a, b, (((1,), (0,)), ((), ())), preferred_element_type=F32)


def dot_t(a, b):
    return lax.dot_general(a, b, (((1,), (1,)), ((), ())), preferred_element_type=F32)


def head_kernel(scale, x_ref, c_ref, ra_ref, rb_ref, wk_ref, wv_ref, dkv_ref, dr_ref, kx_ref, v_ref, q_ref, p_ref, ds_ref):
    n_src, _, tok, width = x_ref.shape
    seq = n_src * tok
    n_blk = seq // Q_BLK
    scale2 = scale * LOG2E
    x = x_ref[...].reshape(seq, width)
    c = c_ref[...]
    k_all = dot(c, jnp.concatenate([wk_ref[0], wk_ref[1]], axis=-1)).astype(BF16)
    v_all = dot(c, jnp.concatenate([wv_ref[0], wv_ref[1]], axis=-1)).astype(BF16)
    v_ref[...] = v_all
    lane = lax.broadcasted_iota(jnp.int32, (Q_BLK, 128), 1)
    for a in range(2):
        cols = slice(a * 128, (a + 1) * 128)
        kx_ref[...] = jnp.concatenate([k_all[:, cols], (ra_ref, rb_ref)[a][...]], axis=-1)
        q_ref[...] = jnp.concatenate([x[:, cols], x[:, 512:640]], axis=-1)
        do = x[:, 256 + a * 128:384 + a * 128]
        for i in range(n_blk):
            top = (i + 1) * Q_BLK
            rows = slice(i * Q_BLK, top)
            s = dot_t(kx_ref[:top, :], q_ref[rows, :]) * scale2
            key = lax.broadcasted_iota(jnp.int32, (top, Q_BLK), 0)
            qry = lax.broadcasted_iota(jnp.int32, (top, Q_BLK), 1) + i * Q_BLK
            s = jnp.where(key <= qry, s, -1e30)
            e = jnp.exp2(s - jnp.max(s, axis=0, keepdims=True))
            p = e / jnp.sum(e, axis=0, keepdims=True)
            dp = dot_t(v_ref[:top, cols], do[rows, :])
            delta = jnp.sum(p * dp, axis=0, keepdims=True)
            p_ref[:top, rows] = p.astype(BF16)
            ds_ref[:top, rows] = (p * (dp - delta) * scale).astype(BF16)
        for j in range(n_blk):
            rows = slice(j * Q_BLK, (j + 1) * Q_BLK)
            dkv_ref[0, 1, rows, cols] = dot(p_ref[rows, j * Q_BLK:], do[j * Q_BLK:, :]).astype(BF16)
            dk = dot(ds_ref[rows, j * Q_BLK:], q_ref[j * Q_BLK:, :])
            dkv_ref[0, 0, rows, cols] = dk[:, :128].astype(BF16)
            half = dk[:, 128:]
            if a == 0:
                dr_ref[0, rows, :] = half
            else:
                dr_ref[0, rows, :] = jnp.where(lane < 64, dr_ref[0, rows, :], half)


def head_part(scale, x, c, ra, rb, wk, wv):
    n_src, pairs, tok, width = x.shape
    seq = n_src * tok
    full = lambda s: pl.BlockSpec(s, lambda p: (0,) * len(s))
    return pl.pallas_call(
        functools.partial(head_kernel, scale),
        grid=(pairs,),
        in_specs=[
            pl.BlockSpec((n_src, 1, tok, width), lambda p: (0, p, 0, 0)),
            full(c.shape), full(ra.shape), full(rb.shape),
            pl.BlockSpec((2, 512, 128), lambda p: (p, 0, 0)),
            pl.BlockSpec((2, 512, 128), lambda p: (p, 0, 0)),
        ],
        out_specs=[
            pl.BlockSpec((1, 2, seq, 256), lambda p: (p, 0, 0, 0)),
            pl.BlockSpec((1, seq, 128), lambda p: (p, 0, 0)),
        ],
        out_shape=[
            jax.ShapeDtypeStruct((pairs, 2, seq, 256), BF16),
            jax.ShapeDtypeStruct((pairs, seq, 128), F32),
        ],
        scratch_shapes=[
            pltpu.VMEM((seq, 256), BF16), pltpu.VMEM((seq, 256), BF16), pltpu.VMEM((seq, 256), BF16),
            pltpu.VMEM((seq, seq), BF16), pltpu.VMEM((seq, seq), BF16),
        ],
        cost_estimate=pl.CostEstimate(flops=6_000_000_000 * pairs // 2, bytes_accessed=8_000_000, transcendentals=0),
        name="head_part",
    )(x, c, ra, rb, wk, wv)


def query_kernel(scale, x_ref, c_ref, ra_ref, rb_ref, wk_ref, wv_ref, o_ref, dq_ref):
    tok = x_ref.shape[1]
    seq = c_ref.shape[0]
    scale2 = scale * LOG2E
    c = c_ref[...]
    k_all = dot(c, jnp.concatenate([wk_ref[0], wk_ref[1]], axis=-1)).astype(BF16)
    v_all = dot(c, jnp.concatenate([wv_ref[0], wv_ref[1]], axis=-1)).astype(BF16)
    me = lax.axis_index("cp")
    key = lax.broadcasted_iota(jnp.int32, (tok, seq), 1)
    qry = lax.broadcasted_iota(jnp.int32, (tok, seq), 0) + me * tok
    rope = None
    for a in range(2):
        cols = slice(a * 128, (a + 1) * 128)
        kx = jnp.concatenate([k_all[:, cols], (ra_ref, rb_ref)[a][...]], axis=-1)
        q = jnp.concatenate([x_ref[0, :, cols], x_ref[0, :, 512:640]], axis=-1)
        do = x_ref[0, :, 256 + a * 128:384 + a * 128]
        s = jnp.where(key <= qry, dot_t(q, kx) * scale2, -1e30)
        e = jnp.exp2(s - jnp.max(s, axis=1, keepdims=True))
        p = e / jnp.sum(e, axis=1, keepdims=True)
        v = v_all[:, cols]
        o_ref[0, :, cols] = dot(p.astype(BF16), v).astype(BF16)
        dp = dot_t(do, v)
        ds = (p * (dp - jnp.sum(p * dp, axis=1, keepdims=True)) * scale).astype(BF16)
        dq = dot(ds, kx)
        dq_ref[0, :, cols] = dq[:, :128].astype(BF16)
        rope = dq[:, 128:] if a == 0 else rope + dq[:, 128:]
    dq_ref[0, :, 256:] = rope.astype(BF16)


def query_part(scale, x, c, ra, rb, wk, wv):
    pairs, tok, width = x.shape
    full = lambda s: pl.BlockSpec(s, lambda p: (0,) * len(s))
    return pl.pallas_call(
        functools.partial(query_kernel, scale),
        grid=(pairs,),
        in_specs=[
            pl.BlockSpec((1, tok, width), lambda p: (p, 0, 0)),
            full(c.shape), full(ra.shape), full(rb.shape),
            pl.BlockSpec((2, 512, 128), lambda p: (p, 0, 0)),
            pl.BlockSpec((2, 512, 128), lambda p: (p, 0, 0)),
        ],
        out_specs=[
            pl.BlockSpec((1, tok, 256), lambda p: (p, 0, 0)),
            pl.BlockSpec((1, tok, 384), lambda p: (p, 0, 0)),
        ],
        out_shape=[
            jax.ShapeDtypeStruct((pairs, tok, 256), BF16),
            jax.ShapeDtypeStruct((pairs, tok, 384), BF16),
        ],
        cost_estimate=pl.CostEstimate(flops=60_000_000_000, bytes_accessed=50_000_000, transcendentals=0),
        name="query_part",
    )(x, c, ra, rb, wk, wv)


def weight_kernel(tok, n_in, *refs):
    dkv_ref, ct_ref, wk_ref, wv_ref = refs[:4]
    dwk_ref, dwv_ref, dc_ref = refs[n_in:n_in + 3]
    me = lax.axis_index("cp")
    n_pair = dkv_ref.shape[0]
    own = pl.ds(pl.multiple_of(me * tok, tok), tok)
    dc = jnp.zeros(dc_ref.shape, F32)
    for which, (w_ref, out_ref) in enumerate(((wk_ref, dwk_ref), (wv_ref, dwv_ref))):
        flat = out_ref.reshape(512 * 8, 128)
        for p in range(n_pair):
            g = dkv_ref[p, which]
            for m in range(4):
                res = dot(ct_ref[m * 128:(m + 1) * 128, :], g)
                for a in range(2):
                    flat[pl.ds(m * 1024 + 2 * p + a, 128, stride=8), :] = res[:, a * 128:(a + 1) * 128]
            mine = dkv_ref[p, which, own, :]
            dc += dot_t(mine, jnp.concatenate([w_ref[2 * p], w_ref[2 * p + 1]], axis=-1))

    @pl.when(pl.program_id(0) == 0)
    def _():
        dc_ref[...] = dc

    @pl.when(pl.program_id(0) > 0)
    def _():
        dc_ref[...] += dc


def weight_part(tok, first, dkv, ct, wk, wv, prev):
    pairs, _, seq, _ = dkv.shape
    steps = pairs // 4
    base = first // 8
    out_block = pl.BlockSpec((512, 8, 128), lambda g: (0, base + g, 0))
    in_specs = [
        pl.BlockSpec((4, 2, seq, 256), lambda g: (g, 0, 0, 0)),
        pl.BlockSpec((512, seq), lambda g: (0, 0)),
        pl.BlockSpec((8, 512, 128), lambda g: (base + g, 0, 0)),
        pl.BlockSpec((8, 512, 128), lambda g: (base + g, 0, 0)),
    ]
    args = [dkv, ct, wk, wv]
    aliases = {}
    if prev is not None:
        in_specs += [pl.BlockSpec(memory_space=pl.ANY)] * 2
        args += list(prev)
        aliases = {4: 0, 5: 1}
    return pl.pallas_call(
        functools.partial(weight_kernel, tok, len(args)),
        grid=(steps,),
        in_specs=in_specs,
        out_specs=[out_block, out_block, pl.BlockSpec((tok, 512), lambda g: (0, 0))],
        out_shape=[
            jax.ShapeDtypeStruct((512, 128, 128), F32),
            jax.ShapeDtypeStruct((512, 128, 128), F32),
            jax.ShapeDtypeStruct((tok, 512), F32),
        ],
        input_output_aliases=aliases,
        cost_estimate=pl.CostEstimate(flops=2_200_000_000 * steps, bytes_accessed=10_000_000 * steps, transcendentals=0),
        name="weight_part",
    )(*args)


def solution(mesh):
    n_dev = mesh.shape["cp"]
    seq_spec = P("cp")

    def local_step(queries, latent, key_rope, w_uk, w_uv, d_out):
        tok, heads, qk = queries.shape
        scale = 1.0 / math.sqrt(qk)
        pairs = heads // 2
        me = lax.axis_index("cp")

        def pair_major(a):
            return a.reshape(tok, pairs, -1).transpose(1, 0, 2)

        payload = jnp.concatenate(
            [pair_major(queries[:, :, :128]), pair_major(d_out), pair_major(queries[:, :, 128:])], axis=-1)
        cr = lax.all_gather(jnp.concatenate([latent, key_rope], axis=-1), "cp", tiled=True)
        c_all, r_all = cr[:, :512], cr[:, 512:]
        zero = jnp.zeros_like(r_all)
        ra = jnp.concatenate([r_all, zero], axis=-1)
        rb = jnp.concatenate([zero, r_all], axis=-1)

        per = pairs // (N_CHUNK * n_dev)
        chunked = payload.reshape(N_CHUNK, n_dev, per, tok, 640)
        gathered = []
        dr = None
        for j in range(N_CHUNK):
            x = lax.all_to_all(chunked[j], "cp", 0, 0, tiled=True)
            start = j * (heads // N_CHUNK) + me * (2 * per)
            wk = lax.dynamic_slice_in_dim(w_uk, start, 2 * per, 1).transpose(1, 0, 2)
            wv = lax.dynamic_slice_in_dim(w_uv, start, 2 * per, 1).transpose(1, 0, 2)
            dkv, dr_j = head_part(scale, x, c_all, ra, rb, wk, wv)
            gathered.append(lax.all_gather(dkv, "cp", tiled=True))
            dr_j = jnp.sum(dr_j, axis=0)
            dr = dr_j if dr is None else dr + dr_j
        dr = (dr[:, :64] + dr[:, 64:]).reshape(n_dev, tok, 64)
        d_key_rope = jnp.sum(lax.all_to_all(dr, "cp", 0, 0, tiled=True), axis=0).astype(BF16)

        wk_h = w_uk.transpose(1, 0, 2)
        wv_h = w_uv.transpose(1, 0, 2)
        o_p, dq_p = query_part(scale, payload, c_all, ra, rb, wk_h, wv_h)
        attn_out = o_p.transpose(1, 0, 2).reshape(tok, heads, 128)
        dq_n = dq_p[:, :, :256].transpose(1, 0, 2).reshape(tok, heads, 128)
        dq_r = dq_p[:, :, 256:].transpose(1, 0, 2).reshape(tok, heads, 64)
        d_query = jnp.concatenate([dq_n, dq_r], axis=-1)

        ct = c_all.T
        prev = None
        dc = None
        for j in range(N_CHUNK):
            dwk, dwv, dc_j = weight_part(tok, j * (heads // N_CHUNK), gathered[j], ct, wk_h, wv_h, prev)
            prev = (dwk, dwv)
            dc = dc_j if dc is None else dc + dc_j
        return attn_out, d_query, dc.astype(BF16), d_key_rope, prev[0], prev[1]

    return jax.shard_map(local_step, mesh=mesh,
                         in_specs=(seq_spec, seq_spec, seq_spec, P(), P(), seq_spec),
                         out_specs=(seq_spec, seq_spec, seq_spec, seq_spec, P(), P()),
                         check_vma=False)
```

```python
import functools
import math
import jax
import jax.numpy as jnp
from jax import lax
from jax.experimental import pallas as pl
from jax.experimental.pallas import tpu as pltpu
from jax.sharding import PartitionSpec as P

N_DEV = 16
TOK = 64
SEQ = 1024
PAIRS = 64
OWN = 4
Q_BLK = 256
LOG2E = 1.4426950408889634
F32 = jnp.float32
BF16 = jnp.bfloat16
MESH = pl.DeviceIdType.MESH
CORE, AX, AY, AZ = 1, 2, 4, 8
ORDERS = ((AX, AY, AZ), (AY, AZ, AX), (AZ, AX, AY))
ROWS = ((0, 336), (336, 336), (672, 352))
CHIPS = (0, 2, 4, 6, 8, 10, 12, 14)


def dot(a, b):
    return lax.dot_general(a, b, (((1,), (0,)), ((), ())), preferred_element_type=F32)


def dot_t(a, b):
    return lax.dot_general(a, b, (((1,), (1,)), ((), ())), preferred_element_type=F32)


def flip(me, mask):
    out = me
    for bit in (1, 2, 4, 8):
        if mask & bit:
            out = out + bit - 2 * bit * ((me // bit) % 2)
    return out


def pack_kernel(q_ref, do_ref, pay_ref, qn_ref, qr_ref, ds_ref):
    step = pl.program_id(0)

    @pl.when(step == 0)
    def _():
        def token(t, carry):
            rows = pl.ds(pl.multiple_of(t * 128, 128), 128)
            qt = q_ref[t].astype(F32)
            qn_ref[rows, :] = qt[0:128, :].T
            qr_ref[rows, 0:64] = qt[128:192, :].T
            ds_ref[rows, :] = do_ref[t].astype(F32)
            return carry
        lax.fori_loop(0, TOK, token, 0, unroll=4)

    for p in range(8):
        head = (step * 8 + p) * 2
        rope = []
        for a in range(2):
            rows = pl.ds(head + a, TOK, stride=128)
            pay_ref[p, :, a * 128:(a + 1) * 128] = qn_ref[rows, :].astype(BF16)
            pay_ref[p, :, 256 + a * 128:384 + a * 128] = ds_ref[rows, :].astype(BF16)
            rope.append(qr_ref[rows, :][:, 0:64])
        pay_ref[p, :, 512:640] = jnp.concatenate(rope, axis=-1).astype(BF16)


def pack(q_t, d_out):
    return pl.pallas_call(
        pack_kernel,
        grid=(8,),
        in_specs=[
            pl.BlockSpec((TOK, 192, 128), lambda s: (0, 0, 0)),
            pl.BlockSpec((TOK, 128, 128), lambda s: (0, 0, 0)),
        ],
        out_specs=pl.BlockSpec((8, TOK, 640), lambda s: (s, 0, 0)),
        out_shape=jax.ShapeDtypeStruct((PAIRS, TOK, 640), BF16),
        scratch_shapes=[pltpu.VMEM((TOK * 128, 128), F32)] * 3,
        cost_estimate=pl.CostEstimate(flops=8_000_000_000, bytes_accessed=11_000_000, transcendentals=0),
        name="pack",
    )(q_t, d_out)


def head_pair(scale, pp, x, c, ropes, wk, wv, out, dr_ref, kx_ref, v_ref, q_ref, p_ref, ds_ref):
    n_blk = SEQ // Q_BLK
    scale2 = scale * LOG2E
    k_all = dot(c, wk).astype(BF16)
    v_ref[...] = dot(c, wv).astype(BF16)
    lane = lax.broadcasted_iota(jnp.int32, (Q_BLK, 128), 1)
    key = lax.broadcasted_iota(jnp.int32, (Q_BLK, Q_BLK), 0)
    qry = lax.broadcasted_iota(jnp.int32, (Q_BLK, Q_BLK), 1)
    for a in range(2):
        cols = slice(a * 128, (a + 1) * 128)
        kx_ref[...] = jnp.concatenate([k_all[:, cols], ropes[a]], axis=-1)
        q_ref[...] = jnp.concatenate([x[:, cols], x[:, 512:640]], axis=-1)
        do = x[:, 256 + a * 128:384 + a * 128]
        for i in range(n_blk):
            top = (i + 1) * Q_BLK
            rows = slice(i * Q_BLK, top)
            s = dot_t(kx_ref[:top, :], q_ref[rows, :]) * scale2
            diag = jnp.where(key <= qry, s[i * Q_BLK:, :], -1e30)
            s = diag if i == 0 else jnp.concatenate([s[:i * Q_BLK, :], diag], axis=0)
            e = jnp.exp2(s - jnp.max(s, axis=0, keepdims=True))
            p = e / jnp.sum(e, axis=0, keepdims=True)
            dp = dot_t(v_ref[:top, cols], do[rows, :])
            delta = jnp.sum(p * dp, axis=0, keepdims=True)
            p_ref[:top, rows] = p.astype(BF16)
            ds_ref[:top, rows] = (p * (dp - delta) * scale).astype(BF16)
        for j in range(n_blk):
            rows = slice(j * Q_BLK, (j + 1) * Q_BLK)
            out[1, rows, cols] = dot(p_ref[rows, j * Q_BLK:], do[j * Q_BLK:, :]).astype(BF16)
            dk = dot(ds_ref[rows, j * Q_BLK:], q_ref[j * Q_BLK:, :])
            out[0, rows, cols] = dk[:, :128].astype(BF16)
            keep = lane < 64 if a == 0 else lane >= 64
            dr_ref[rows, :] = dr_ref[rows, :] + jnp.where(keep, dk[:, 128:], 0.0)


def query_pair(scale, me, x, c, ropes, wk, wv):
    scale2 = scale * LOG2E
    k_all = dot(c, wk).astype(BF16)
    v_all = dot(c, wv).astype(BF16)
    key = lax.broadcasted_iota(jnp.int32, (TOK, SEQ), 1)
    qry = lax.broadcasted_iota(jnp.int32, (TOK, SEQ), 0) + me * TOK
    outs, grads = [], []
    for a in range(2):
        cols = slice(a * 128, (a + 1) * 128)
        kx = jnp.concatenate([k_all[:, cols], ropes[a]], axis=-1)
        q = jnp.concatenate([x[:, cols], x[:, 512:640]], axis=-1)
        do = x[:, 256 + a * 128:384 + a * 128]
        s = jnp.where(key <= qry, dot_t(q, kx) * scale2, -1e30)
        e = jnp.exp2(s - jnp.max(s, axis=1, keepdims=True))
        p = e / jnp.sum(e, axis=1, keepdims=True)
        v = v_all[:, cols]
        outs.append(dot(p.astype(BF16), v))
        dp = dot_t(do, v)
        ds = (p * (dp - jnp.sum(p * dp, axis=1, keepdims=True)) * scale).astype(BF16)
        grads.append(dot(ds, kx))
    return outs, grads


def mega_kernel(scale, pay, cr, wk, wv,
                dkv, wt_out, o_out, dq_out, dr_out, c_out,
                xbuf, cbuf, rb, wnat, wt, stage, kx, vs, qs, ps, dss, dr_acc, dr_land, xq, osc, dqn, dqr,
                c_send, c_recv, c_sib, x_send, x_recv, ici_send, ici_recv, sib_send, sib_recv,
                dr_send, dr_recv, load_sem, wsem, xq_sem, wt_sem, st_sem):
    me = lax.axis_index("cp")
    core = me % 2
    chip = me // 2
    sib = flip(me, CORE)
    bar = pltpu.get_barrier_semaphore()
    for m in range(1, N_DEV):
        pl.semaphore_signal(bar, inc=1, device_id=(flip(me, m),), device_id_type=MESH)
    pl.semaphore_wait(bar, N_DEV - 1)

    def remote(src, dst, ssem, rsem, to):
        return pltpu.make_async_remote_copy(src_ref=src, dst_ref=dst, send_sem=ssem, recv_sem=rsem,
                                            device_id=(to,), device_id_type=MESH)

    for m in CHIPS[1:]:
        remote(cr, cbuf.at[chip, core], c_send, c_recv, flip(me, m)).start()
    own_c = pltpu.make_async_copy(cr, cbuf.at[chip, core], load_sem.at[0])
    own_c.start()
    own_w = []
    for i, w in enumerate((wk, wv)):
        cp = pltpu.make_async_copy(w.at[:, pl.ds(pl.multiple_of(me * 8, 8), 8), :], wnat.at[0, i], wsem.at[0, i])
        cp.start()
        own_w.append(cp)
    for pp in range(OWN):
        for m in range(1, N_DEV):
            to = flip(me, m)
            remote(pay.at[OWN * to + pp], xbuf.at[pp, me], x_send, x_recv.at[pp], to).start()
    own_x = pltpu.make_async_copy(pay.at[pl.ds(OWN * me, OWN)], xbuf.at[:, me], load_sem.at[1])
    own_x.start()

    dr_acc[...] = jnp.zeros_like(dr_acc)
    for cp in own_w:
        cp.wait()
    for i in range(2):
        wt[0, i] = jnp.transpose(wnat[0, i], (1, 0, 2))
    own_c.wait()
    arrived = cbuf.at[pl.ds(0, 7), 0]
    pltpu.make_async_copy(arrived, arrived, c_recv).wait()
    fwd = remote(cbuf.at[:, core], cbuf.at[:, core], c_send, c_sib, sib)
    fwd.start()
    fwd.wait_recv()

    def latent():
        return cbuf[...].reshape(SEQ, 640)

    rope_a = latent()[:, 512:640].astype(F32)
    rb[...] = pltpu.roll(rope_a, 64, axis=1).astype(BF16)

    def operands():
        cc = latent()
        return cc[:, :512], (cc[:, 512:640], rb[...])

    own_x.wait()

    def block(mask, p, k):
        return dkv.at[OWN * flip(me, mask) + p, :, pl.ds(ROWS[k][0], ROWS[k][1]), :]

    def to_sibling(mask, p, k):
        b = block(mask, p, k)
        remote(b, b, sib_send, sib_recv, sib).start()

    def known(k, s):
        masks = [0]
        for d in ORDERS[k][:s]:
            masks = masks + [m + d for m in masks]
        return masks

    def gather_stage(p, s):
        for k in range(3):
            if s > 0:
                d = ORDERS[k][s - 1]
                for m in known(k, s - 1):
                    b = block(m + d, p, k)
                    pltpu.make_async_copy(b, b, ici_recv.at[p, k, (m + d) // 2]).wait()
            if s < 3:
                d = ORDERS[k][s]
                for m in known(k, s):
                    b = block(m, p, k)
                    remote(b, b, ici_send, ici_recv.at[p, k, (m + d) // 2], flip(me, d)).start()
        for k in range(3):
            fresh = [0] if s == 0 else [m + ORDERS[k][s - 1] for m in known(k, s - 1)]
            for m in fresh:
                to_sibling(m, p, k)

    def head_step(pp, carry):
        got = xbuf.at[pp, pl.ds(0, N_DEV - 1)]
        pltpu.make_async_copy(got, got, x_recv.at[pp]).wait()
        x = xbuf[pp].reshape(SEQ, 640)
        c, ropes = operands()
        wkp = jnp.concatenate([wt[0, 0, 2 * pp], wt[0, 0, 2 * pp + 1]], axis=-1)
        wvp = jnp.concatenate([wt[0, 1, 2 * pp], wt[0, 1, 2 * pp + 1]], axis=-1)
        head_pair(scale, pp, x, c, ropes, wkp, wvp, stage, dr_acc, kx, vs, qs, ps, dss)
        cp = pltpu.make_async_copy(stage, dkv.at[OWN * me + pp], st_sem)
        cp.start()
        cp.wait()
        for p in range(OWN):
            @pl.when(pp == p)
            def _():
                gather_stage(p, 0)
        return carry

    lax.fori_loop(0, OWN, head_step, 0)

    for m in range(1, N_DEV):
        to = flip(me, m)
        remote(dr_acc.at[pl.ds(pl.multiple_of(to * TOK, TOK), TOK), :], dr_land.at[me], dr_send, dr_recv, to).start()
    own_dr = pltpu.make_async_copy(dr_acc.at[pl.ds(pl.multiple_of(me * TOK, TOK), TOK), :], dr_out, load_sem.at[2])
    own_dr.start()

    def fetch(g, slot):
        cps = [pltpu.make_async_copy(w.at[:, pl.ds(pl.multiple_of(g * 8, 8), 8), :], wnat.at[slot, i], wsem.at[slot, i])
               for i, w in enumerate((wk, wv))]
        cps.append(pltpu.make_async_copy(pay.at[pl.ds(g * 4, 4)], xq.at[slot], xq_sem.at[slot]))
        return cps

    def put_w(g, slot):
        return pltpu.make_async_copy(wt.at[slot], wt_out.at[:, pl.ds(pl.multiple_of(g * 8, 8), 8)], wt_sem.at[slot])

    for cp in fetch(0, 0):
        cp.start()

    plan = {0: ((0, 1),), 1: ((1, 1),), 2: ((2, 1),), 4: ((0, 2),), 6: ((3, 1),), 8: ((1, 2),), 10: ((2, 2),), 12: ((3, 2),)}

    def query_step(g, carry):
        slot = g % 2
        for cp in fetch(g, slot):
            cp.wait()

        @pl.when(g < 15)
        def _():
            for cp in fetch(g + 1, 1 - slot):
                cp.start()

        @pl.when(g >= 2)
        def _():
            put_w(g - 2, slot).wait()

        for i in range(2):
            wt[slot, i] = jnp.transpose(wnat[slot, i], (1, 0, 2))
        put_w(g, slot).start()

        def pair_step(j, carry):
            x = xq[slot, j]
            c, ropes = operands()
            wkp = jnp.concatenate([wt[slot, 0, 2 * j], wt[slot, 0, 2 * j + 1]], axis=-1)
            wvp = jnp.concatenate([wt[slot, 1, 2 * j], wt[slot, 1, 2 * j + 1]], axis=-1)
            outs, grads = query_pair(scale, me, x, c, ropes, wkp, wvp)
            for a in range(2):
                osc[pl.ds(2 * j + a, TOK, stride=8), :] = outs[a]
                rows = pl.ds(g * 8 + 2 * j + a, TOK, stride=128)
                dqn[rows, :] = grads[a][:, :128]
                rope = grads[a][:, 128:]
                dqr[rows, :] = rope if a == 0 else pltpu.roll(rope, 64, axis=1)
            return carry

        lax.fori_loop(0, 4, pair_step, 0)
        o_out[:, pl.ds(pl.multiple_of(g * 8, 8), 8), :] = osc[...].reshape(TOK, 8, 128).astype(BF16)
        for when, events in plan.items():
            @pl.when(g == when)
            def _():
                for p, s in events:
                    gather_stage(p, s)
        return carry

    lax.fori_loop(0, 16, query_step, 0)

    def dq_token(t, carry):
        rows = pl.ds(pl.multiple_of(t * 128, 128), 128)
        dq_out[t, 0:128, :] = dqn[rows, :].T.astype(BF16)
        dq_out[t, 128:192, :] = dqr[rows, :].T[0:64, :].astype(BF16)
        return carry

    lax.fori_loop(0, TOK, dq_token, 0)
    c_out[...] = latent()[:, :512]
    for p in range(OWN):
        gather_stage(p, 3)

    own_dr.wait()
    got = dr_land.at[pl.ds(0, N_DEV - 1)]
    pltpu.make_async_copy(got, got, dr_recv).wait()
    total = dr_out[...]
    for m in range(1, N_DEV):
        total = total + dr_land[flip(me, m)]
    dr_out[...] = total

    put_w(14, 0).wait()
    put_w(15, 1).wait()
    pltpu.make_async_copy(got, got, dr_send).wait()
    got = xbuf.at[:, pl.ds(0, N_DEV - 1)]
    pltpu.make_async_copy(got, got, x_send).wait()
    arrived = cbuf.at[pl.ds(0, 7), 0]
    pltpu.make_async_copy(arrived, arrived, c_send).wait()
    arrived = cbuf.at[:, 0]
    pltpu.make_async_copy(arrived, arrived, c_send).wait()
    sent = dkv.at[pl.ds(0, 7 * OWN)]
    pltpu.make_async_copy(sent, sent, ici_send).wait()
    sent = dkv.at[pl.ds(0, 8 * OWN)]
    pltpu.make_async_copy(sent, sent, sib_send).wait()
    pltpu.make_async_copy(sent, sent, sib_recv).wait()


def mega(scale, pay, cr, wk, wv):
    any_spec = pl.BlockSpec(memory_space=pl.ANY)
    vmem = pl.BlockSpec(memory_space=pltpu.VMEM)
    dma = pltpu.SemaphoreType.DMA
    return pl.pallas_call(
        functools.partial(mega_kernel, scale),
        in_specs=[any_spec] * 4,
        out_specs=[any_spec, any_spec, vmem, vmem, vmem, vmem],
        out_shape=[
            jax.ShapeDtypeStruct((PAIRS, 2, SEQ, 256), BF16),
            jax.ShapeDtypeStruct((2, 128, 512, 128), BF16),
            jax.ShapeDtypeStruct((TOK, 128, 128), BF16),
            jax.ShapeDtypeStruct((TOK, 192, 128), BF16),
            jax.ShapeDtypeStruct((TOK, 128), F32),
            jax.ShapeDtypeStruct((SEQ, 512), BF16),
        ],
        scratch_shapes=[
            pltpu.VMEM((OWN, N_DEV, TOK, 640), BF16),
            pltpu.VMEM((8, 2, TOK, 640), BF16),
            pltpu.VMEM((SEQ, 128), BF16),
            pltpu.VMEM((2, 2, 512, 8, 128), BF16),
            pltpu.VMEM((2, 2, 8, 512, 128), BF16),
            pltpu.VMEM((2, SEQ, 256), BF16),
            pltpu.VMEM((SEQ, 256), BF16), pltpu.VMEM((SEQ, 256), BF16), pltpu.VMEM((SEQ, 256), BF16),
            pltpu.VMEM((SEQ, SEQ), BF16), pltpu.VMEM((SEQ, SEQ), BF16),
            pltpu.VMEM((SEQ, 128), F32),
            pltpu.VMEM((N_DEV, TOK, 128), F32),
            pltpu.VMEM((2, 4, TOK, 640), BF16),
            pltpu.VMEM((TOK * 8, 128), F32),
            pltpu.VMEM((TOK * 128, 128), F32), pltpu.VMEM((TOK * 128, 128), F32),
            dma, dma, dma, dma, dma((OWN,)), dma, dma((OWN, 3, 8)), dma, dma,
            dma, dma, dma((3,)), dma((2, 2)), dma((2,)), dma((2,)), dma,
        ],
        compiler_params=pltpu.CompilerParams(collective_id=0, has_side_effects=True, vmem_limit_bytes=60 * 1024 * 1024),
        cost_estimate=pl.CostEstimate(flops=100_000_000_000, bytes_accessed=200_000_000, transcendentals=0),
        name="mega",
    )(pay, cr, wk, wv)


def weight_kernel(dkv_ref, ct_ref, wt_ref, dwk_ref, dwv_ref, dc_ref):
    me = lax.axis_index("cp")
    n_pair = dkv_ref.shape[0]
    own = pl.ds(pl.multiple_of(me * TOK, TOK), TOK)
    dc = jnp.zeros(dc_ref.shape, F32)
    for which, out_ref in enumerate((dwk_ref, dwv_ref)):
        flat = out_ref.reshape(512 * 8, 128)
        for p in range(n_pair):
            g = dkv_ref[p, which]
            for m in range(2):
                res = dot(ct_ref[m * 256:(m + 1) * 256, :], g)
                for a in range(2):
                    flat[pl.ds(m * 2048 + 2 * p + a, 256, stride=8), :] = res[:, a * 128:(a + 1) * 128]
            mine = dkv_ref[p, which, own, :]
            dc += dot_t(mine, jnp.concatenate([wt_ref[which, 2 * p], wt_ref[which, 2 * p + 1]], axis=-1))

    @pl.when(pl.program_id(0) == 0)
    def _():
        dc_ref[...] = dc

    @pl.when(pl.program_id(0) > 0)
    def _():
        dc_ref[...] += dc


def weight_part(dkv, ct, wt):
    out_block = pl.BlockSpec((512, 8, 128), lambda g: (0, g, 0))
    return pl.pallas_call(
        weight_kernel,
        grid=(PAIRS // 4,),
        in_specs=[
            pl.BlockSpec((4, 2, SEQ, 256), lambda g: (g, 0, 0, 0)),
            pl.BlockSpec((512, SEQ), lambda g: (0, 0)),
            pl.BlockSpec((2, 8, 512, 128), lambda g: (0, g, 0, 0)),
        ],
        out_specs=[out_block, out_block, pl.BlockSpec((TOK, 512), lambda g: (0, 0))],
        out_shape=[
            jax.ShapeDtypeStruct((512, 128, 128), F32),
            jax.ShapeDtypeStruct((512, 128, 128), F32),
            jax.ShapeDtypeStruct((TOK, 512), F32),
        ],
        cost_estimate=pl.CostEstimate(flops=36_000_000_000, bytes_accessed=170_000_000, transcendentals=0),
        name="weight_part",
    )(dkv, ct, wt)


def solution(mesh):
    seq_spec = P("cp")

    def local_step(queries, latent, key_rope, w_uk, w_uv, d_out):
        scale = 1.0 / math.sqrt(queries.shape[-1])
        pay = pack(queries.transpose(0, 2, 1), d_out)
        cr = jnp.concatenate([latent, key_rope, jnp.zeros_like(key_rope)], axis=-1)
        dkv, wt, o, dq, dr, c_all = mega(scale, pay, cr, w_uk, w_uv)
        dwk, dwv, dc = weight_part(dkv, c_all.T, wt)
        d_key_rope = (dr[:, :64] + dr[:, 64:]).astype(BF16)
        return o, dq.transpose(0, 2, 1), dc.astype(BF16), d_key_rope, dwk, dwv

    return jax.shard_map(local_step, mesh=mesh,
                         in_specs=(seq_spec, seq_spec, seq_spec, P(), P(), seq_spec),
                         out_specs=(seq_spec, seq_spec, seq_spec, seq_spec, P(), P()),
                         check_vma=False)
```

```python
import functools
import math
import jax
import jax.numpy as jnp
from jax import lax
from jax.experimental import pallas as pl
from jax.experimental.pallas import tpu as pltpu
from jax.sharding import PartitionSpec as P

N_DEV = 16
TOK = 64
SEQ = 1024
PAIRS = 64
OWN = 4
Q_BLK = 256
LANE = 128
WIDE = 256
LAT = 512
PACK = 640
ROPE = 64
SUB = 8
VMEM_ALL = 67_000_000
LOG2E = 1.4426950408889634
F32 = jnp.float32
BF16 = jnp.bfloat16
MESH = pl.DeviceIdType.MESH
CORE, AX, AY, AZ = 1, 2, 4, 8
ORDERS = ((AX, AY, AZ), (AY, AZ, AX), (AZ, AX, AY))
ROWS = ((0, 336), (336, 336), (672, 352))
CHIPS = (0, 2, 4, 6, 8, 10, 12, 14)
LATE = (2, 3)
PITCH = 136
PEERS = (14, 2, 4, 8, 15, 3, 5, 9, 6, 12, 10, 7, 13, 11, 1)


def dot(a, b):
    return lax.dot_general(a, b, (((1,), (0,)), ((), ())), preferred_element_type=F32)


def dot_t(a, b):
    return lax.dot_general(a, b, (((1,), (1,)), ((), ())), preferred_element_type=F32)


def flip(me, mask):
    out = me
    for bit in (1, 2, 4, SUB):
        if mask & bit:
            out = out + bit - 2 * bit * ((me // bit) % 2)
    return out


def place(dev):
    return (dev % 2) * SUB + dev // 2


def known(k, s):
    masks = [0]
    for d in ORDERS[k][:s]:
        masks = masks + [m + d for m in masks]
    return masks


def pack_kernel(q_ref, do_ref, pay_ref, qn_ref, qr_ref, ds_ref):
    step = pl.program_id(0)

    @pl.when(step == 0)
    def _():
        def token(t, carry):
            rows = pl.ds(pl.multiple_of(t * PITCH, SUB), LANE)
            qt = q_ref[t].astype(F32)
            qn_ref[rows, :] = qt[0:LANE, :].T
            qr_ref[rows, 0:ROPE] = qt[LANE:192, :].T
            ds_ref[rows, :] = do_ref[t].astype(F32)
            return carry
        lax.fori_loop(0, TOK, token, 0, unroll=4)

    for p in range(SUB):
        head = (step * SUB + p) * 2
        rope = []
        for a in range(2):
            rows = pl.ds(head + a, TOK, stride=PITCH)
            pay_ref[p, :, a * LANE:(a + 1) * LANE] = qn_ref[rows, :].astype(BF16)
            pay_ref[p, :, WIDE + a * LANE:384 + a * LANE] = ds_ref[rows, :].astype(BF16)
            rope.append(qr_ref[rows, :][:, 0:ROPE])
        pay_ref[p, :, LAT:PACK] = jnp.concatenate(rope, axis=-1).astype(BF16)


def pack(q_t, d_out):
    return pl.pallas_call(
        pack_kernel,
        grid=(SUB,),
        in_specs=[
            pl.BlockSpec((TOK, 192, LANE), lambda s: (0, 0, 0)),
            pl.BlockSpec((TOK, LANE, LANE), lambda s: (0, 0, 0)),
        ],
        out_specs=pl.BlockSpec((SUB, TOK, PACK), lambda s: (s, 0, 0)),
        out_shape=jax.ShapeDtypeStruct((PAIRS, TOK, PACK), BF16),
        scratch_shapes=[pltpu.VMEM((TOK * PITCH, LANE), F32)] * 3,
        cost_estimate=pl.CostEstimate(flops=8_000_000_000, bytes_accessed=11_000_000, transcendentals=0),
        name="pack",
    )(q_t, d_out)


def head_pair(scale, pp, x, c, ropes, wk, wv, out, dr_ref, kx_ref, v_ref, q_ref, p_ref, ds_ref):
    n_blk = SEQ // Q_BLK
    scale2 = scale * LOG2E
    k_all = dot(c, wk).astype(BF16)
    v_ref[...] = dot(c, wv).astype(BF16)
    lane = lax.broadcasted_iota(jnp.int32, (Q_BLK, LANE), 1)
    key = lax.broadcasted_iota(jnp.int32, (Q_BLK, Q_BLK), 0)
    qry = lax.broadcasted_iota(jnp.int32, (Q_BLK, Q_BLK), 1)
    for a in range(2):
        cols = slice(a * LANE, (a + 1) * LANE)
        kx_ref[...] = jnp.concatenate([k_all[:, cols], ropes[a]], axis=-1)
        q_ref[...] = jnp.concatenate([x[:, cols], x[:, LAT:PACK]], axis=-1)
        do = x[:, WIDE + a * LANE:384 + a * LANE]
        for i in range(n_blk):
            top = (i + 1) * Q_BLK
            rows = slice(i * Q_BLK, top)
            s = dot_t(kx_ref[:top, :], q_ref[rows, :]) * scale2
            diag = jnp.where(key <= qry, s[i * Q_BLK:, :], -1e30)
            s = diag if i == 0 else jnp.concatenate([s[:i * Q_BLK, :], diag], axis=0)
            e = jnp.exp2(s - jnp.max(s, axis=0, keepdims=True))
            p = e / jnp.sum(e, axis=0, keepdims=True)
            dp = dot_t(v_ref[:top, cols], do[rows, :])
            delta = jnp.sum(p * dp, axis=0, keepdims=True)
            p_ref[:top, rows] = p.astype(BF16)
            ds_ref[:top, rows] = (p * (dp - delta) * scale).astype(BF16)
        for j in range(n_blk):
            rows = slice(j * Q_BLK, (j + 1) * Q_BLK)
            out[1, rows, cols] = dot(p_ref[rows, j * Q_BLK:], do[j * Q_BLK:, :]).astype(BF16)
            dk = dot(ds_ref[rows, j * Q_BLK:], q_ref[j * Q_BLK:, :])
            out[0, rows, cols] = dk[:, :LANE].astype(BF16)
            keep = lane < ROPE if a == 0 else lane >= ROPE
            dr_ref[rows, :] = dr_ref[rows, :] + jnp.where(keep, dk[:, LANE:], 0.0)


def query_pair(scale, me, x, k_all, v_all, r):
    scale2 = scale * LOG2E
    z = jnp.zeros((TOK, LANE), BF16)

    def diagonal(u):
        return jnp.concatenate([jnp.concatenate([u[:, :LANE], z], axis=1), jnp.concatenate([z, u[:, LANE:]], axis=1)], axis=0)

    q_rope = jnp.concatenate([x[:, LAT:576], x[:, 576:PACK]], axis=0)
    s = (dot_t(k_all, diagonal(x[:, :WIDE])) + dot_t(r[:, :ROPE], q_rope)) * scale2
    key = lax.broadcasted_iota(jnp.int32, (SEQ, LANE), 0)
    qry = lax.broadcasted_iota(jnp.int32, (SEQ, LANE), 1) % TOK + me * TOK
    s = jnp.where(key <= qry, s, -1e30)
    e = jnp.exp2(s - jnp.max(s, axis=0, keepdims=True))
    p = e / jnp.sum(e, axis=0, keepdims=True)
    dp = dot_t(v_all, diagonal(x[:, WIDE:LAT]))
    ds = (p * (dp - jnp.sum(p * dp, axis=0, keepdims=True)) * scale).astype(BF16).T
    o = dot(p.astype(BF16).T, v_all)
    dq = dot(ds, k_all)
    dq_rope = dot(ds, r)
    halves = (slice(0, TOK), slice(TOK, 2 * TOK))
    return [(o[h, c], dq[h, c], dq_rope[h, :]) for h, c in zip(halves, (slice(0, LANE), slice(LANE, WIDE)))]


def mega_kernel(scale, pay, cr, wk, wv,
                dkv, s20, s21, s22, s30, s31, s32, n20, n21, n22, n30, n31, n32, wt_out, o_out, dq_out, dr_out, ct_out, dc_out,
                xbuf, cbuf, rb, wnat, wt, kv, stage, kx, vs, qs, ps, dss, dr_acc, dr_land, xq, grow, osc, dqn, dqr,
                c_send, c_recv, c_sib, x_send, x_recv, ici_send, ici_recv, sib_send, sib_recv,
                dr_send, dr_recv, load_sem, own_sem, wsem, xq_sem, wt_sem, st_sem):
    me = lax.axis_index("cp")
    core = me % 2
    chip = me // 2
    sib = flip(me, CORE)
    late = {2: (s20, s21, s22), 3: (s30, s31, s32)}
    late_sib = {2: (n20, n21, n22), 3: (n30, n31, n32)}
    bar = pltpu.get_barrier_semaphore()
    for m in range(1, N_DEV):
        pl.semaphore_signal(bar, inc=1, device_id=(flip(me, m),), device_id_type=MESH)
    pl.semaphore_wait(bar, N_DEV - 1)

    def remote(src, dst, ssem, rsem, to):
        return pltpu.make_async_remote_copy(src_ref=src, dst_ref=dst, send_sem=ssem, recv_sem=rsem,
                                            device_id=(to,), device_id_type=MESH)

    for m in CHIPS[1:]:
        remote(cr, cbuf.at[chip, core], c_send, c_recv, flip(me, m)).start()
    own_c = pltpu.make_async_copy(cr, cbuf.at[chip, core], load_sem.at[0])
    own_c.start()
    own_w = []
    for i, w in enumerate((wk, wv)):
        for pp in range(2):
            first = pl.multiple_of(32 * pp + SUB * (place(me) // 4), SUB)
            own_w.append(pltpu.make_async_copy(w.at[:, pl.ds(first, SUB), :], wnat.at[pp, i], wsem.at[pp, i]))
            own_w[-1].start()
    for pp in range(OWN):
        for m in PEERS:
            to = flip(me, m)
            remote(pay.at[16 * pp + place(to)], xbuf.at[pp, me], x_send, x_recv.at[pp], to).start()
    own_x = [pltpu.make_async_copy(pay.at[16 * pp + place(me)], xbuf.at[pp, me], own_sem.at[pp]) for pp in range(OWN)]
    for cp in own_x:
        cp.start()

    dr_acc[...] = jnp.zeros_like(dr_acc)
    for cp in own_w:
        cp.wait()
    for i in range(2):
        for pp in range(2):
            wt[pp, i] = jnp.transpose(wnat[pp, i], (1, 0, 2))
    own_c.wait()
    arrived = cbuf.at[pl.ds(0, 7), 0]
    pltpu.make_async_copy(arrived, arrived, c_recv).wait()
    fwd = remote(cbuf.at[:, core], cbuf.at[:, core], c_send, c_sib, sib)
    fwd.start()
    fwd.wait_recv()

    def latent():
        return cbuf[...].reshape(SEQ, PACK)

    rope_a = latent()[:, LAT:PACK].astype(F32)
    rb[...] = pltpu.roll(rope_a, ROPE, axis=1).astype(BF16)

    def operands():
        cc = latent()
        return cc[:, :LAT], (cc[:, LAT:PACK], rb[...])

    for cp in own_x:
        cp.wait()

    def block(mask, p, k):
        if p in LATE:
            return late[p][k].at[known(k, 2).index(mask)]
        return dkv.at[16 * p + place(flip(me, mask)), :, pl.ds(ROWS[k][0], ROWS[k][1]), :]

    def to_sibling(mask, p, k):
        b = block(mask, p, k)
        there = late_sib[p][k].at[known(k, 2).index(mask)] if p in LATE else b
        remote(b, there, sib_send, sib_recv.at[p], sib).start()

    def gather_stage(p, s):
        last = 2 if p in LATE else 3
        fresh = [[0] if s == 0 else [m + ORDERS[k][s - 1] for m in known(k, s - 1)] for k in range(3)]

        def arrive(k, m):
            b = block(m, p, k)
            pltpu.make_async_copy(b, b, ici_recv.at[p, k, m // 2]).wait()

        if s == last:
            for j in range(len(fresh[0])):
                for k in range(3):
                    arrive(k, fresh[k][j])
                    to_sibling(fresh[k][j], p, k)
            return
        for k in range(3):
            if s > 0:
                for m in fresh[k]:
                    arrive(k, m)
            d = ORDERS[k][s]
            for m in known(k, s):
                there = block(m + d, p, k) if p in LATE else block(m, p, k)
                remote(block(m, p, k), there, ici_send, ici_recv.at[p, k, (m + d) // 2], flip(me, d)).start()
        for k in range(3):
            for m in fresh[k]:
                to_sibling(m, p, k)

    def own_heads(pp):
        return [pltpu.make_async_copy(
            w.at[:, pl.ds(pl.multiple_of(32 * pp + SUB * (place(me) // 4), SUB), SUB), :], wnat.at[pp % 2, i], wsem.at[pp % 2, i])
            for i, w in enumerate((wk, wv))]

    for pp in range(2, OWN):
        for cp in own_heads(pp):
            cp.start()
    first = 2 * (place(me) % 4)

    def head_step(pp, carry):
        got = xbuf.at[pp, pl.ds(0, N_DEV - 1)]
        pltpu.make_async_copy(got, got, x_recv.at[pp]).wait()
        x = xbuf[pp].reshape(SEQ, PACK)
        c, ropes = operands()
        slot = pp % 2
        wkp = jnp.concatenate([wt[slot, 0, first], wt[slot, 0, first + 1]], axis=-1)
        wvp = jnp.concatenate([wt[slot, 1, first], wt[slot, 1, first + 1]], axis=-1)
        head_pair(scale, pp, x, c, ropes, wkp, wvp, stage, dr_acc, kx, vs, qs, ps, dss)

        for p in range(OWN):
            @pl.when(pp == p)
            def _():
                cps = []
                if p in LATE:
                    for k in range(3):
                        cps.append(pltpu.make_async_copy(
                            stage.at[:, pl.ds(ROWS[k][0], ROWS[k][1]), :], late[p][k].at[0], st_sem.at[k]))
                else:
                    cps.append(pltpu.make_async_copy(stage, dkv.at[16 * p + place(me)], st_sem.at[0]))
                for cp in cps:
                    cp.start()
                for cp in cps:
                    cp.wait()
                gather_stage(p, 0)
                if p < 2:
                    for cp in own_heads(p + 2):
                        cp.wait()
                    for i in range(2):
                        wt[p, i] = jnp.transpose(wnat[p, i], (1, 0, 2))
        return carry

    lax.fori_loop(0, OWN, head_step, 0)

    for m in range(1, N_DEV):
        to = flip(me, m)
        remote(dr_acc.at[pl.ds(pl.multiple_of(to * TOK, TOK), TOK), :], dr_land.at[me], dr_send, dr_recv, to).start()
    own_dr = pltpu.make_async_copy(dr_acc.at[pl.ds(pl.multiple_of(me * TOK, TOK), TOK), :], dr_out, load_sem.at[2])
    own_dr.start()

    def fetch(g, slot):
        cps = [pltpu.make_async_copy(w.at[:, pl.ds(pl.multiple_of(g * SUB, SUB), SUB), :], wnat.at[slot, i], wsem.at[slot, i])
               for i, w in enumerate((wk, wv))]
        cps.append(pltpu.make_async_copy(pay.at[pl.ds(g * 4, 4)], xq.at[slot], xq_sem.at[slot]))
        return cps

    def put_w(g, slot):
        return pltpu.make_async_copy(wt.at[slot], wt_out.at[:, pl.ds(pl.multiple_of(g * SUB, SUB), SUB)], wt_sem.at[slot])

    for cp in fetch(0, 0):
        cp.start()

    plan = {1: ((0, 1),), 2: ((1, 1),), 6: ((0, 2),), SUB: ((1, 2),), 9: ((2, 1),), 10: ((3, 1),)}

    def query_step(g, carry):
        slot = g % 2
        for cp in fetch(g, slot):
            cp.wait()

        @pl.when(g < 15)
        def _():
            for cp in fetch(g + 1, 1 - slot):
                cp.start()

        @pl.when(g >= 2)
        def _():
            put_w(g - 2, slot).wait()

        for i in range(2):
            wt[slot, i] = jnp.transpose(wnat[slot, i], (1, 0, 2))
        put_w(g, slot).start()

        def project(j):
            c = latent()[:, :LAT]
            for i in range(2):
                kv[j % 2, i] = dot(c, jnp.concatenate([wt[slot, i, 2 * j], wt[slot, i, 2 * j + 1]], axis=-1)).astype(BF16)

        project(0)
        for j in range(4):
            if j < 3:
                project(j + 1)
            r = latent()[:, LAT:PACK]
            res = query_pair(scale, me, xq[slot, j], kv[j % 2, 0], kv[j % 2, 1], r)
            for a in range(2):
                o, dq, dq_rope = res[a]
                osc[pl.ds(2 * j + a, TOK, stride=SUB), :] = o
                rows = pl.ds(g * SUB + 2 * j + a, TOK, stride=PITCH)
                dqn[rows, :] = dq
                dqr[rows, :] = dq_rope
        o_out[:, pl.ds(pl.multiple_of(g * SUB, SUB), SUB), :] = osc[...].reshape(TOK, SUB, LANE).astype(BF16)
        for when, events in plan.items():
            @pl.when(g == when)
            def _():
                for p, s in events:
                    gather_stage(p, s)
        return carry

    lax.fori_loop(0, 16, query_step, 0)

    def dq_token(t, carry):
        rows = pl.ds(pl.multiple_of(t * PITCH, SUB), LANE)
        dq_out[t, 0:LANE, :] = dqn[rows, :].T.astype(BF16)
        dq_out[t, LANE:192, :] = dqr[rows, :].T[0:ROPE, :].astype(BF16)
        return carry

    lax.fori_loop(0, TOK, dq_token, 0)
    ct_out[...] = latent()[:, :LAT].T
    put_w(14, 0).wait()
    put_w(15, 1).wait()
    for p in range(OWN):
        if p not in LATE:
            gather_stage(p, 3)
    for p in range(OWN):
        if p not in LATE:
            got = dkv.at[pl.ds(16 * p, SUB)]
            pltpu.make_async_copy(got, got, sib_recv.at[p]).wait()

    own = pl.ds(pl.multiple_of(me * TOK, TOK), TOK)

    def rows_of(t, slot):
        return [pltpu.make_async_copy(wt_out.at[:, pl.ds(pl.multiple_of(t * SUB, SUB), SUB)], wt.at[slot], wt_sem.at[slot]),
                pltpu.make_async_copy(dkv.at[pl.ds(4 * t, 4), :, own, :], grow.at[slot], xq_sem.at[slot])]

    for cp in rows_of(0, 0):
        cp.start()
    dc_out[...] = jnp.zeros_like(dc_out)

    def dc_step(t, carry):
        slot = t % 2
        for cp in rows_of(t, slot):
            cp.wait()

        @pl.when(t < 7)
        def _():
            for cp in rows_of(t + 1, 1 - slot):
                cp.start()

        for i in range(2):
            for j in range(4):
                w = jnp.concatenate([wt[slot, i, 2 * j], wt[slot, i, 2 * j + 1]], axis=-1)
                dc_out[...] += dot_t(grow[slot, j, i], w)
        return carry

    lax.fori_loop(0, SUB, dc_step, 0)
    for p in LATE:
        gather_stage(p, 2)

    own_dr.wait()
    got = dr_land.at[pl.ds(0, N_DEV - 1)]
    pltpu.make_async_copy(got, got, dr_recv).wait()
    total = dr_out[...]
    for m in range(1, N_DEV):
        total = total + dr_land[flip(me, m)]
    dr_out[...] = total

    pltpu.make_async_copy(got, got, dr_send).wait()
    got = xbuf.at[:, pl.ds(0, N_DEV - 1)]
    pltpu.make_async_copy(got, got, x_send).wait()
    arrived = cbuf.at[pl.ds(0, 7), 0]
    pltpu.make_async_copy(arrived, arrived, c_send).wait()
    arrived = cbuf.at[:, 0]
    pltpu.make_async_copy(arrived, arrived, c_send).wait()
    sent = dkv.at[pl.ds(0, 20)]
    pltpu.make_async_copy(sent, sent, ici_send).wait()
    sent = dkv.at[pl.ds(0, 24)]
    pltpu.make_async_copy(sent, sent, sib_send).wait()
    for p in LATE:
        got = dkv.at[pl.ds(0, 4)]
        pltpu.make_async_copy(got, got, sib_recv.at[p]).wait()


def mega(scale, pay, cr, wk, wv):
    any_spec = pl.BlockSpec(memory_space=pl.ANY)
    vmem = pl.BlockSpec(memory_space=pltpu.VMEM)
    dma = pltpu.SemaphoreType.DMA
    return pl.pallas_call(
        functools.partial(mega_kernel, scale),
        in_specs=[any_spec] * 4,
        out_specs=[any_spec] * 14 + [vmem] * 5,
        out_shape=[
            jax.ShapeDtypeStruct((32, 2, SEQ, WIDE), BF16),
            *[jax.ShapeDtypeStruct((4, 2, n, WIDE), BF16) for _ in range(4) for _, n in ROWS],
            jax.ShapeDtypeStruct((2, LANE, LAT, LANE), BF16),
            jax.ShapeDtypeStruct((TOK, LANE, LANE), BF16),
            jax.ShapeDtypeStruct((TOK, 192, LANE), BF16),
            jax.ShapeDtypeStruct((TOK, LANE), F32),
            jax.ShapeDtypeStruct((LAT, SEQ), BF16),
            jax.ShapeDtypeStruct((TOK, LAT), F32),
        ],
        scratch_shapes=[
            pltpu.VMEM((OWN, N_DEV, TOK, PACK), BF16),
            pltpu.VMEM((SUB, 2, TOK, PACK), BF16),
            pltpu.VMEM((SEQ, LANE), BF16),
            pltpu.VMEM((2, 2, LAT, SUB, LANE), BF16),
            pltpu.VMEM((2, 2, SUB, LAT, LANE), BF16),
            pltpu.VMEM((2, 2, SEQ, WIDE), BF16),
            pltpu.VMEM((2, SEQ, WIDE), BF16),
            pltpu.VMEM((SEQ, WIDE), BF16), pltpu.VMEM((SEQ, WIDE), BF16), pltpu.VMEM((SEQ, WIDE), BF16),
            pltpu.VMEM((SEQ, SEQ), BF16), pltpu.VMEM((SEQ, SEQ), BF16),
            pltpu.VMEM((SEQ, LANE), F32),
            pltpu.VMEM((N_DEV, TOK, LANE), F32),
            pltpu.VMEM((2, 4, TOK, PACK), BF16),
            pltpu.VMEM((2, 4, 2, TOK, WIDE), BF16),
            pltpu.VMEM((TOK * SUB, LANE), F32),
            pltpu.VMEM((TOK * PITCH, LANE), F32), pltpu.VMEM((TOK * PITCH, LANE), F32),
            dma, dma, dma, dma, dma((OWN,)), dma, dma((OWN, 3, SUB)), dma, dma((OWN,)),
            dma, dma, dma((3,)), dma((OWN,)), dma((2, 2)), dma((2,)), dma((2,)), dma((3,)),
        ],
        compiler_params=pltpu.CompilerParams(collective_id=0, has_side_effects=True, vmem_limit_bytes=VMEM_ALL),
        cost_estimate=pl.CostEstimate(flops=100_000_000_000, bytes_accessed=200_000_000, transcendentals=0),
        name="mega",
    )(pay, cr, wk, wv)


def weight_kernel(dkv_ref, ct_ref, dwk_ref, dwv_ref):
    for which, out_ref in enumerate((dwk_ref, dwv_ref)):
        flat = out_ref.reshape(LAT * SUB, LANE)
        for p in range(4):
            g = dkv_ref[p, which]
            for m in range(2):
                res = dot(ct_ref[m * WIDE:(m + 1) * WIDE, :], g)
                for a in range(2):
                    flat[pl.ds(m * 2048 + 2 * p + a, WIDE, stride=SUB), :] = res[:, a * LANE:(a + 1) * LANE]


def weight_part(dkv, ct):
    out_block = pl.BlockSpec((LAT, SUB, LANE), lambda g: (0, g, 0))
    return pl.pallas_call(
        weight_kernel,
        grid=(SUB,),
        in_specs=[
            pl.BlockSpec((4, 2, SEQ, WIDE), lambda g: (g, 0, 0, 0)),
            pl.BlockSpec((LAT, SEQ), lambda g: (0, 0)),
        ],
        out_specs=[out_block, out_block],
        out_shape=[jax.ShapeDtypeStruct((LAT, LANE, LANE), F32)] * 2,
        compiler_params=pltpu.CompilerParams(vmem_limit_bytes=VMEM_ALL),
        cost_estimate=pl.CostEstimate(flops=18_000_000_000, bytes_accessed=70_000_000, transcendentals=0),
        name="weight_part",
    )(dkv, ct)


def late_kernel(p, other, with_rows, *refs):
    near, far = refs[0:3], refs[3:6]
    ct, wt, _, _, dc_in = refs[6:11]
    carry = ()
    if with_rows:
        o_in, dq_in, dwk, dwv, dc_out, o_out, dq_out, dc_acc, gbuf, wbuf, obuf, gsem, wsem, osem, o_buf, dq_buf, csem = refs[11:]
        carry = ((o_in, o_buf, o_out), (dq_in, dq_buf, dq_out))
    else:
        dwk, dwv, dc_out, dc_acc, gbuf, wbuf, obuf, gsem, wsem, osem = refs[11:]
    me = lax.axis_index("cp")
    src = flip(me, CORE) if other else me
    own = pl.ds(pl.multiple_of(me * TOK, TOK), TOK)
    tiles = [4 * p + place(flip(src, AZ * b)) // 4 for b in range(2)]
    for b in range(2):
        for i in range(2):
            for j in range(4):
                mask = AZ * b + 2 * j
                for k in range(3):
                    d = ORDERS[k][2]
                    ref, m = (far[k], mask - d) if mask & d else (near[k], mask)
                    pltpu.make_async_copy(ref.at[known(k, 2).index(m), i],
                                          gbuf.at[b, i, j, pl.ds(ROWS[k][0], ROWS[k][1]), :], gsem.at[b, i]).start()
            pltpu.make_async_copy(wt.at[i, pl.ds(pl.multiple_of(tiles[b] * SUB, SUB), SUB)], wbuf.at[b, i], wsem.at[b, i]).start()
    if carry:
        moves = []
        for n, (src_ref, buf, dst_ref) in enumerate(carry):
            cp = pltpu.make_async_copy(src_ref, buf, csem.at[n])
            cp.start()
            moves.append((cp, pltpu.make_async_copy(buf, dst_ref, csem.at[n])))
    dc_acc[...] = dc_in[...]

    def store(b, i, tile):
        where = (dwk, dwv)[i].at[:, pl.ds(pl.multiple_of(tile * SUB, SUB), SUB), :]
        return pltpu.make_async_copy(obuf.at[b, i].reshape(LAT, SUB, LANE), where, osem.at[b, i])

    x, y = (src // AX) % 2, (src // AY) % 2

    def half_tile(n, carried):
        b, i = n // 2, n % 2
        pltpu.make_async_copy(gbuf.at[b, i], gbuf.at[b, i], gsem.at[b, i]).wait()
        pltpu.make_async_copy(wbuf.at[b, i], wbuf.at[b, i], wsem.at[b, i]).wait()
        for j in range(4):
            dx, dy = j % 2, j // 2
            slot = 2 * (2 * (y + dy - 2 * y * dy) + x + dx - 2 * x * dx)
            dc_acc[...] += dot_t(gbuf[b, i, j, own, :], jnp.concatenate([wbuf[b, i, slot], wbuf[b, i, slot + 1]], axis=-1))
            for m in range(2):
                res = dot(ct[m * WIDE:(m + 1) * WIDE, :], gbuf[b, i, j])
                for a in range(2):
                    obuf[b, i, pl.ds(m * 2048 + slot + a, WIDE, stride=SUB), :] = res[:, a * LANE:(a + 1) * LANE]
        tile = tiles[0] + b * (tiles[1] - tiles[0])
        for which in range(2):
            @pl.when(i == which)
            def _():
                store(b, which, tile).start()
        return carried

    lax.fori_loop(0, 4, half_tile, 0)
    dc_out[...] = dc_acc[...].astype(dc_out.dtype)
    if carry:
        for load, put in moves:
            load.wait()
            put.start()
        for load, put in moves:
            put.wait()
    for b in range(2):
        for i in range(2):
            store(b, i, tiles[b]).wait()


def late_part(p, other, last, near, far, ct, wt, dwk, dwv, dc, rows=()):
    any_spec = pl.BlockSpec(memory_space=pl.ANY)
    vmem = pl.BlockSpec(memory_space=pltpu.VMEM)
    dma = pltpu.SemaphoreType.DMA
    shapes = [jax.ShapeDtypeStruct(r.shape, r.dtype) for r in rows]
    return pl.pallas_call(
        functools.partial(late_kernel, p, other, bool(rows)),
        in_specs=[any_spec] * 6 + [vmem, any_spec, any_spec, any_spec, vmem] + [any_spec] * len(rows),
        out_specs=[any_spec, any_spec, vmem] + [any_spec] * len(rows),
        out_shape=[
            jax.ShapeDtypeStruct((LAT, LANE, LANE), F32),
            jax.ShapeDtypeStruct((LAT, LANE, LANE), F32),
            jax.ShapeDtypeStruct((TOK, LAT), BF16 if last else F32),
            *shapes,
        ],
        scratch_shapes=[
            pltpu.VMEM((TOK, LAT), F32),
            pltpu.VMEM((2, 2, 4, SEQ, WIDE), BF16),
            pltpu.VMEM((2, 2, SUB, LAT, LANE), BF16),
            pltpu.VMEM((2, 2, 4096, LANE), F32),
            dma((2, 2)), dma((2, 2)), dma((2, 2)),
            *([pltpu.VMEM(r.shape, r.dtype) for r in rows] + [dma((2,))] if rows else []),
        ],
        input_output_aliases={SUB: 0, 9: 1},
        compiler_params=pltpu.CompilerParams(vmem_limit_bytes=VMEM_ALL),
        cost_estimate=pl.CostEstimate(flops=4_500_000_000, bytes_accessed=20_000_000, transcendentals=0),
        name=f"late_part_{p}_{int(other)}",
    )(*near, *far, ct, wt, dwk, dwv, dc, *rows)


def solution(mesh):
    seq_spec = P("cp")

    def local_step(queries, latent, key_rope, w_uk, w_uv, d_out):
        scale = 1.0 / math.sqrt(queries.shape[-1])
        pay = pack(queries.transpose(0, 2, 1), d_out)
        cr = jnp.concatenate([latent, key_rope, jnp.zeros_like(key_rope)], axis=-1)
        dkv, *late, wt, o, dq, dr, ct, dc = mega(scale, pay, cr, w_uk, w_uv)
        mine = {p: late[3 * i:3 * i + 3] for i, p in enumerate(LATE)}
        sibs = {p: late[6 + 3 * i:9 + 3 * i] for i, p in enumerate(LATE)}

        def swap(a, d):
            return lax.ppermute(a, "cp", [(i, i ^ d) for i in range(N_DEV)])

        far = {p: [swap(a, ORDERS[k][2]) for k, a in enumerate(mine[p])] for p in LATE}
        grads = (*weight_part(dkv, ct), dc)
        for p in LATE:
            got, grads = lax.optimization_barrier((far[p], grads))
            got_sib = [swap(a, CORE) for a in got]
            grads = late_part(p, False, False, mine[p], got, ct, wt, *grads)
            first = p == LATE[0]
            res = late_part(p, True, p == LATE[-1], sibs[p], got_sib, ct, wt, *grads, rows=(o, dq) if first else ())
            grads = res[:3]
            if first:
                o, dq = res[3:]
        dwk, dwv, dc = grads
        d_key_rope = (dr[:, :ROPE] + dr[:, ROPE:]).astype(BF16)
        return o, dq.transpose(0, 2, 1), dc, d_key_rope, dwk, dwv

    return jax.shard_map(local_step, mesh=mesh,
                         in_specs=(seq_spec, seq_spec, seq_spec, P(), P(), seq_spec),
                         out_specs=(seq_spec, seq_spec, seq_spec, seq_spec, P(), P()),
                         check_vma=False)
```

```python
import functools
import math
import jax
import jax.numpy as jnp
from jax import lax
from jax.experimental import pallas as pl
from jax.experimental.pallas import tpu as pltpu
from jax.sharding import PartitionSpec as P

N_DEV = 16
TOK = 64
SEQ = 1024
PAIRS = 64
OWN = 4
Q_BLK = 256
LANE = 128
WIDE = 256
LAT = 512
PACK = 640
ROPE = 64
SUB = 8
VMEM_ALL = 67_000_000
LOG2E = 1.4426950408889634
F32 = jnp.float32
BF16 = jnp.bfloat16
MESH = pl.DeviceIdType.MESH
CORE, AX, AY, AZ = 1, 2, 4, 8
ORDERS = ((AX, AY, AZ), (AY, AZ, AX), (AZ, AX, AY))
ROWS = ((0, 336), (336, 336), (672, 352))
BOTH = 2048
CHIPS = (0, 2, 4, 6, 8, 10, 12, 14)
LATE = (2, 3)
PITCH = 136
PEERS = (14, 2, 4, 8, 15, 3, 5, 9, 6, 12, 10, 7, 13, 11, 1)


def dot(a, b):
    return lax.dot_general(a, b, (((1,), (0,)), ((), ())), preferred_element_type=F32)


def dot_t(a, b):
    return lax.dot_general(a, b, (((1,), (1,)), ((), ())), preferred_element_type=F32)


def flip(me, mask):
    out = me
    for bit in (1, 2, 4, SUB):
        if mask & bit:
            out = out + bit - 2 * bit * ((me // bit) % 2)
    return out


def place(dev):
    return (dev % 2) * SUB + dev // 2


def known(k, s):
    masks = [0]
    for d in ORDERS[k][:s]:
        masks = masks + [m + d for m in masks]
    return masks


def segments(which, lo, hi):
    parts = []
    for start, n in ROWS:
        a, b = max(lo, start), min(hi, start + n)
        if a < b:
            parts.append((a, b - a, start + which * n + a))
    return parts


def head_pair(scale, pp, x, c, ropes, wk, wv, out, dr_ref, kx_ref, v_ref, q_ref, p_ref, ds_ref):
    n_blk = SEQ // Q_BLK
    scale2 = scale * LOG2E
    k_all = dot(c, wk).astype(BF16)
    v_ref[...] = dot(c, wv).astype(BF16)
    lane = lax.broadcasted_iota(jnp.int32, (Q_BLK, LANE), 1)
    key = lax.broadcasted_iota(jnp.int32, (Q_BLK, Q_BLK), 0)
    qry = lax.broadcasted_iota(jnp.int32, (Q_BLK, Q_BLK), 1)
    for a in range(2):
        cols = slice(a * LANE, (a + 1) * LANE)
        kx_ref[...] = jnp.concatenate([k_all[:, cols], ropes[a]], axis=-1)
        q_ref[...] = jnp.concatenate([x[:, cols], x[:, LAT:PACK]], axis=-1)
        do = x[:, WIDE + a * LANE:384 + a * LANE]
        for i in range(n_blk):
            top = (i + 1) * Q_BLK
            rows = slice(i * Q_BLK, top)
            s = dot_t(kx_ref[:top, :], q_ref[rows, :]) * scale2
            diag = jnp.where(key <= qry, s[i * Q_BLK:, :], -1e30)
            s = diag if i == 0 else jnp.concatenate([s[:i * Q_BLK, :], diag], axis=0)
            e = jnp.exp2(s - jnp.max(s, axis=0, keepdims=True))
            p = e * (1.0 / jnp.sum(e, axis=0, keepdims=True))
            dp = dot_t(v_ref[:top, cols], do[rows, :])
            delta = jnp.sum(p * dp, axis=0, keepdims=True)
            p_ref[:top, rows] = p.astype(BF16)
            ds_ref[:top, rows] = (p * (dp - delta)).astype(BF16)
        for j in range(n_blk):
            rows = slice(j * Q_BLK, (j + 1) * Q_BLK)
            dv = dot(p_ref[rows, j * Q_BLK:], do[j * Q_BLK:, :]).astype(BF16)
            dk = dot(ds_ref[rows, j * Q_BLK:], q_ref[j * Q_BLK:, :]) * scale
            for which, grad in enumerate((dk[:, :LANE].astype(BF16), dv)):
                for row, n, at in segments(which, j * Q_BLK, (j + 1) * Q_BLK):
                    out[at:at + n, cols] = grad[row - j * Q_BLK:row - j * Q_BLK + n, :]
            keep = lane < ROPE if a == 0 else lane >= ROPE
            dr_ref[rows, :] = dr_ref[rows, :] + jnp.where(keep, dk[:, LANE:], 0.0)


def query_pair(scale, me, x, k_all, v_all, r):
    scale2 = scale * LOG2E
    z = jnp.zeros((TOK, LANE), BF16)

    def diagonal(u):
        return jnp.concatenate([jnp.concatenate([u[:, :LANE], z], axis=1), jnp.concatenate([z, u[:, LANE:]], axis=1)], axis=0)

    q_rope = jnp.concatenate([x[:, LAT:576], x[:, 576:PACK]], axis=0)
    s = (dot_t(k_all, diagonal(x[:, :WIDE])) + dot_t(r[:, :ROPE], q_rope)) * scale2
    key = lax.broadcasted_iota(jnp.int32, (SEQ, LANE), 0)
    qry = lax.broadcasted_iota(jnp.int32, (SEQ, LANE), 1) % TOK + me * TOK
    s = jnp.where(key <= qry, s, -1e30)
    e = jnp.exp2(s - jnp.max(s, axis=0, keepdims=True))
    p = e * (1.0 / jnp.sum(e, axis=0, keepdims=True))
    dp = dot_t(v_all, diagonal(x[:, WIDE:LAT]))
    ds = (p * (dp - jnp.sum(p * dp, axis=0, keepdims=True))).astype(BF16).T
    o = dot(p.astype(BF16).T, v_all)
    dq = dot(ds, k_all) * scale
    dq_rope = dot(ds, r) * scale
    halves = (slice(0, TOK), slice(TOK, 2 * TOK))
    return [(o[h, c], dq[h, c], dq_rope[h, :]) for h, c in zip(halves, (slice(0, LANE), slice(LANE, WIDE)))]


def mega_kernel(scale, q_in, do_in, cr, wk, wv,
                dkv, s20, s21, s22, s30, s31, s32, n20, n21, n22, n30, n31, n32, wt_out, o_out, dq_out, dr_out, ct_out, dc_out,
                xbuf, cbuf, rb, wnat, wt, wt_own, kv, stage, kx, vs, qs, ps, dss, dr_acc, dr_land, pay, grow, osc, dqn, dqr, dos,
                c_send, c_recv, c_sib, x_send, x_recv, ici_send, ici_recv, sib_send, sib_recv,
                dr_send, dr_recv, load_sem, own_sem, wsem, xq_sem, wt_sem, st_sem):
    me = lax.axis_index("cp")
    core = me % 2
    chip = me // 2
    sib = flip(me, CORE)
    late = {2: (s20, s21, s22), 3: (s30, s31, s32)}
    late_sib = {2: (n20, n21, n22), 3: (n30, n31, n32)}
    by_token = [pltpu.make_async_copy(src, dst, own_sem.at[n]) for n, (src, dst) in enumerate(((q_in, dq_out), (do_in, o_out)))]
    for cp in by_token:
        cp.start()
    bar = pltpu.get_barrier_semaphore()
    for m in range(1, N_DEV):
        pl.semaphore_signal(bar, inc=1, device_id=(flip(me, m),), device_id_type=MESH)
    pl.semaphore_wait(bar, N_DEV - 1)

    def remote(src, dst, ssem, rsem, to):
        return pltpu.make_async_remote_copy(src_ref=src, dst_ref=dst, send_sem=ssem, recv_sem=rsem,
                                            device_id=(to,), device_id_type=MESH)

    for m in CHIPS[1:]:
        remote(cr, cbuf.at[chip, core], c_send, c_recv, flip(me, m)).start()
    own_c = pltpu.make_async_copy(cr, cbuf.at[chip, core], load_sem.at[0])
    own_c.start()

    def fetch_tile(tile, slot):
        return [pltpu.make_async_copy(w.at[:, pl.ds(pl.multiple_of(tile * SUB, SUB), SUB), :], wnat.at[slot, i], wsem.at[slot, i])
                for i, w in enumerate((wk, wv))]

    def own_tile(pp):
        return 4 * pp + place(me) // 4

    for pp in range(2):
        for cp in fetch_tile(own_tile(pp), pp):
            cp.start()
    for cp in by_token:
        cp.wait()

    def unpack_token(t, carry):
        rows = pl.ds(pl.multiple_of(t * PITCH, SUB), LANE)
        qt = dq_out[t].astype(F32)
        dqn[rows, :] = qt[:LANE, :].T
        dqr[rows, 0:ROPE] = qt[LANE:, :].T
        dos[rows, :] = o_out[t].astype(F32)
        return carry

    lax.fori_loop(0, TOK, unpack_token, 0, unroll=SUB)

    def pack_pair(p, carry):
        rope = []
        for a in range(2):
            rows = pl.ds(2 * p + a, TOK, stride=PITCH)
            pay[p, :, a * LANE:(a + 1) * LANE] = dqn[rows, :].astype(BF16)
            pay[p, :, (a + 2) * LANE:(a + 3) * LANE] = dos[rows, :].astype(BF16)
            rope.append(dqr[rows, :][:, :ROPE])
        pay[p, :, LAT:] = jnp.concatenate(rope, axis=-1).astype(BF16)
        return carry

    def to_owners(pp):
        for m in PEERS:
            to = flip(me, m)
            remote(pay.at[N_DEV * pp + place(to)], xbuf.at[pp, me], x_send, x_recv.at[pp], to).start()

    for pp in range(OWN):
        lax.fori_loop(N_DEV * pp, N_DEV * (pp + 1), pack_pair, 0, unroll=4)
        if pp:
            to_owners(pp - 1)

    dr_acc[...] = jnp.zeros_like(dr_acc)
    first = 2 * (place(me) % 4)
    for pp in range(OWN):
        for cp in fetch_tile(own_tile(pp), pp % 2):
            cp.wait()
        for i in range(2):
            wt[pp % 2, i] = jnp.transpose(wnat[pp % 2, i], (1, 0, 2))
            wt_own[pp, i] = wt[pp % 2, i, pl.ds(first, 2)]
        for cp in fetch_tile(own_tile(pp + 2), pp) if pp < 2 else fetch_tile(pp - 2, pp - 2):
            cp.start()
        if pp == 0:
            to_owners(OWN - 1)
    own_c.wait()
    arrived = cbuf.at[pl.ds(0, 7), 0]
    pltpu.make_async_copy(arrived, arrived, c_recv).wait()
    fwd = remote(cbuf.at[:, core], cbuf.at[:, core], c_send, c_sib, sib)
    fwd.start()
    fwd.wait_recv()

    def latent():
        return cbuf[...].reshape(SEQ, PACK)

    rope_a = latent()[:, LAT:PACK].astype(F32)
    rb[...] = pltpu.roll(rope_a, ROPE, axis=1).astype(BF16)

    def operands():
        cc = latent()
        return cc[:, :LAT], (cc[:, LAT:PACK], rb[...])

    for pp in range(OWN):
        xbuf[pp, me] = pay[N_DEV * pp + place(me)]

    def block(mask, p, k):
        if p in LATE:
            return late[p][k].at[known(k, 2).index(mask)]
        return dkv.at[N_DEV * p + place(flip(me, mask)), pl.ds(2 * ROWS[k][0], 2 * ROWS[k][1]), :]

    def to_sibling(mask, p, k):
        b = block(mask, p, k)
        there = late_sib[p][k].at[known(k, 2).index(mask)] if p in LATE else b
        remote(b, there, sib_send, sib_recv.at[p], sib).start()

    def gather_stage(p, s):
        last = 2 if p in LATE else 3
        fresh = [[0] if s == 0 else [m + ORDERS[k][s - 1] for m in known(k, s - 1)] for k in range(3)]

        def arrive(k, m):
            b = block(m, p, k)
            pltpu.make_async_copy(b, b, ici_recv.at[p, k, m // 2]).wait()

        if s == last:
            for j in range(len(fresh[0])):
                for k in range(3):
                    arrive(k, fresh[k][j])
                    to_sibling(fresh[k][j], p, k)
            return
        for k in range(3):
            if s > 0:
                for m in fresh[k]:
                    arrive(k, m)
            d = ORDERS[k][s]
            for m in known(k, s):
                there = block(m + d, p, k) if p in LATE else block(m, p, k)
                remote(block(m, p, k), there, ici_send, ici_recv.at[p, k, (m + d) // 2], flip(me, d)).start()
        for k in range(3):
            for m in fresh[k]:
                to_sibling(m, p, k)

    def head_step(pp):
        got = xbuf.at[pp, pl.ds(0, N_DEV - 1)]
        pltpu.make_async_copy(got, got, x_recv.at[pp]).wait()
        x = xbuf[pp].reshape(SEQ, PACK)
        c, ropes = operands()
        wkp = jnp.concatenate([wt_own[pp, 0, 0], wt_own[pp, 0, 1]], axis=-1)
        wvp = jnp.concatenate([wt_own[pp, 1, 0], wt_own[pp, 1, 1]], axis=-1)
        head_pair(scale, pp, x, c, ropes, wkp, wvp, stage, dr_acc, kx, vs, qs, ps, dss)

        for p in range(OWN):
            @pl.when(pp == p)
            def _():
                cps = []
                if p in LATE:
                    for k in range(3):
                        cps.append(pltpu.make_async_copy(
                            stage.at[pl.ds(2 * ROWS[k][0], 2 * ROWS[k][1]), :], late[p][k].at[0], st_sem.at[k]))
                else:
                    cps.append(pltpu.make_async_copy(stage, dkv.at[16 * p + place(me)], st_sem.at[0]))
                for cp in cps:
                    cp.start()
                for cp in cps:
                    cp.wait()
                gather_stage(p, 0)

    own_dr = pltpu.make_async_copy(dr_acc.at[pl.ds(pl.multiple_of(me * TOK, TOK), TOK), :], dr_out, load_sem.at[1])

    def share_rope():
        for m in range(1, N_DEV):
            to = flip(me, m)
            remote(dr_acc.at[pl.ds(pl.multiple_of(to * TOK, TOK), TOK), :], dr_land.at[me], dr_send, dr_recv, to).start()
        own_dr.start()

    def put_w(g, slot):
        return pltpu.make_async_copy(wt.at[slot], wt_out.at[:, pl.ds(pl.multiple_of(g * SUB, SUB), SUB)], wt_sem.at[slot])

    plan = {4: ((0, 1),), 5: ((1, 1),), 9: ((0, 2),), 10: ((1, 2),), 13: ((2, 1),), 15: ((3, 1),)}

    def query_step(g, carry):
        slot = g % 2
        for cp in fetch_tile(g, slot):
            cp.wait()

        @pl.when((g > 0) & (g < 15))
        def _():
            for cp in fetch_tile(g + 1, 1 - slot):
                cp.start()

        @pl.when(g >= 2)
        def _():
            put_w(g - 2, slot).wait()

        for i in range(2):
            wt[slot, i] = jnp.transpose(wnat[slot, i], (1, 0, 2))
        put_w(g, slot).start()

        def project(j):
            c = latent()[:, :LAT]
            for i in range(2):
                kv[j % 2, i] = dot(c, jnp.concatenate([wt[slot, i, 2 * j], wt[slot, i, 2 * j + 1]], axis=-1)).astype(BF16)

        project(0)
        for j in range(4):
            if j < 3:
                project(j + 1)
            r = latent()[:, LAT:PACK]
            res = query_pair(scale, me, pay[4 * g + j], kv[j % 2, 0], kv[j % 2, 1], r)
            for a in range(2):
                o, dq, dq_rope = res[a]
                osc[pl.ds(2 * j + a, TOK, stride=SUB), :] = o
                rows = pl.ds(g * SUB + 2 * j + a, TOK, stride=PITCH)
                dqn[rows, :] = dq
                dqr[rows, :] = dq_rope
        o_out[:, pl.ds(pl.multiple_of(g * SUB, SUB), SUB), :] = osc[...].reshape(TOK, SUB, LANE).astype(BF16)
        @pl.when(g < OWN)
        def _():
            head_step(g)

        @pl.when(g == OWN - 1)
        def _():
            share_rope()

        for when, events in plan.items():
            @pl.when(g == when)
            def _():
                for p, s in events:
                    gather_stage(p, s)
        return carry

    lax.fori_loop(0, 16, query_step, 0)

    def dq_token(t, carry):
        rows = pl.ds(pl.multiple_of(t * PITCH, SUB), LANE)
        dq_out[t, 0:LANE, :] = dqn[rows, :].T.astype(BF16)
        dq_out[t, LANE:192, :] = dqr[rows, :].T[0:ROPE, :].astype(BF16)
        return carry

    lax.fori_loop(0, TOK, dq_token, 0)
    ct_out[...] = latent()[:, :LAT].T
    put_w(14, 0).wait()
    put_w(15, 1).wait()
    for p in range(OWN):
        if p not in LATE:
            gather_stage(p, 3)
    for p in range(OWN):
        if p not in LATE:
            got = dkv.at[pl.ds(16 * p, SUB)]
            pltpu.make_async_copy(got, got, sib_recv.at[p]).wait()

    def rows_of(t, slot):
        cps = [pltpu.make_async_copy(wt_out.at[:, pl.ds(pl.multiple_of(t * SUB, SUB), SUB)], wt.at[slot], wt_sem.at[slot])]
        for n in range(4):
            sixteen = 4 * me + n
            third = sixteen // 21 - sixteen // 63
            for i in range(2):
                at = pl.multiple_of(N_DEV * (sixteen + 21 * third + i * (21 + third // 2)), N_DEV)
                cps.append(pltpu.make_async_copy(dkv.at[pl.ds(4 * t, 4), pl.ds(at, N_DEV), :],
                                                 grow.at[slot, i, :, pl.ds(N_DEV * n, N_DEV), :], xq_sem.at[slot, 4 * i + n]))
        return cps

    for cp in rows_of(0, 0):
        cp.start()
    dc_out[...] = jnp.zeros_like(dc_out)

    def dc_step(t, carry):
        slot = t % 2
        for cp in rows_of(t, slot):
            cp.wait()

        @pl.when(t < 7)
        def _():
            for cp in rows_of(t + 1, 1 - slot):
                cp.start()

        for i in range(2):
            for j in range(4):
                w = jnp.concatenate([wt[slot, i, 2 * j], wt[slot, i, 2 * j + 1]], axis=-1)
                dc_out[...] += dot_t(grow[slot, i, j], w)
        return carry

    lax.fori_loop(0, SUB, dc_step, 0)
    for p in LATE:
        gather_stage(p, 2)

    own_dr.wait()
    got = dr_land.at[pl.ds(0, N_DEV - 1)]
    pltpu.make_async_copy(got, got, dr_recv).wait()
    total = dr_out[...]
    for m in range(1, N_DEV):
        total = total + dr_land[flip(me, m)]
    dr_out[...] = total

    pltpu.make_async_copy(got, got, dr_send).wait()
    got = xbuf.at[:, pl.ds(0, N_DEV - 1)]
    pltpu.make_async_copy(got, got, x_send).wait()
    arrived = cbuf.at[pl.ds(0, 7), 0]
    pltpu.make_async_copy(arrived, arrived, c_send).wait()
    arrived = cbuf.at[:, 0]
    pltpu.make_async_copy(arrived, arrived, c_send).wait()
    sent = dkv.at[pl.ds(0, 20)]
    pltpu.make_async_copy(sent, sent, ici_send).wait()
    sent = dkv.at[pl.ds(0, 24)]
    pltpu.make_async_copy(sent, sent, sib_send).wait()
    for p in LATE:
        got = dkv.at[pl.ds(0, 4)]
        pltpu.make_async_copy(got, got, sib_recv.at[p]).wait()


def mega(scale, q_t, d_out, cr, wk, wv):
    any_spec = pl.BlockSpec(memory_space=pl.ANY)
    vmem = pl.BlockSpec(memory_space=pltpu.VMEM)
    dma = pltpu.SemaphoreType.DMA
    return pl.pallas_call(
        functools.partial(mega_kernel, scale),
        in_specs=[any_spec] * 5,
        out_specs=[any_spec] * 14 + [vmem] * 5,
        out_shape=[
            jax.ShapeDtypeStruct((32, BOTH, WIDE), BF16),
            *[jax.ShapeDtypeStruct((4, 2 * n, WIDE), BF16) for _ in range(4) for _, n in ROWS],
            jax.ShapeDtypeStruct((2, LANE, LAT, LANE), BF16),
            jax.ShapeDtypeStruct((TOK, LANE, LANE), BF16),
            jax.ShapeDtypeStruct((TOK, 192, LANE), BF16),
            jax.ShapeDtypeStruct((TOK, LANE), F32),
            jax.ShapeDtypeStruct((LAT, SEQ), BF16),
            jax.ShapeDtypeStruct((TOK, LAT), F32),
        ],
        scratch_shapes=[
            pltpu.VMEM((OWN, N_DEV, TOK, PACK), BF16),
            pltpu.VMEM((SUB, 2, TOK, PACK), BF16),
            pltpu.VMEM((SEQ, LANE), BF16),
            pltpu.VMEM((2, 2, LAT, SUB, LANE), BF16),
            pltpu.VMEM((2, 2, SUB, LAT, LANE), BF16),
            pltpu.VMEM((OWN, 2, 2, LAT, LANE), BF16),
            pltpu.VMEM((2, 2, SEQ, WIDE), BF16),
            pltpu.VMEM((BOTH, WIDE), BF16),
            pltpu.VMEM((SEQ, WIDE), BF16), pltpu.VMEM((SEQ, WIDE), BF16), pltpu.VMEM((SEQ, WIDE), BF16),
            pltpu.VMEM((SEQ, SEQ), BF16), pltpu.VMEM((SEQ, SEQ), BF16),
            pltpu.VMEM((SEQ, LANE), F32),
            pltpu.VMEM((N_DEV, TOK, LANE), F32),
            pltpu.VMEM((PAIRS, TOK, PACK), BF16),
            pltpu.VMEM((2, 2, 4, TOK, WIDE), BF16),
            pltpu.VMEM((TOK * SUB, LANE), F32),
            *[pltpu.VMEM((TOK * PITCH, LANE), F32)] * 3,
            dma, dma, dma, dma, dma((OWN,)), dma, dma((OWN, 3, SUB)), dma, dma((OWN,)),
            dma, dma, dma((2,)), dma((2,)), dma((2, 2)), dma((2, SUB)), dma((2,)), dma((3,)),
        ],
        compiler_params=pltpu.CompilerParams(collective_id=0, has_side_effects=True, vmem_limit_bytes=VMEM_ALL),
        cost_estimate=pl.CostEstimate(flops=100_000_000_000, bytes_accessed=200_000_000, transcendentals=0),
        name="mega",
    )(q_t, d_out, cr, wk, wv)


def weight_kernel(dkv_ref, ct_ref, dwk_ref, dwv_ref):
    for which, out_ref in enumerate((dwk_ref, dwv_ref)):
        flat = out_ref.reshape(LAT * SUB, LANE)
        for p in range(4):
            g = jnp.concatenate([dkv_ref[p, at:at + n, :] for _, n, at in segments(which, 0, SEQ)], axis=0)
            for m in range(2):
                res = dot(ct_ref[m * WIDE:(m + 1) * WIDE, :], g)
                for a in range(2):
                    flat[pl.ds(m * 2048 + 2 * p + a, WIDE, stride=SUB), :] = res[:, a * LANE:(a + 1) * LANE]


def weight_part(dkv, ct):
    out_block = pl.BlockSpec((LAT, SUB, LANE), lambda g: (0, g, 0))
    return pl.pallas_call(
        weight_kernel,
        grid=(SUB,),
        in_specs=[
            pl.BlockSpec((4, BOTH, WIDE), lambda g: (g, 0, 0)),
            pl.BlockSpec((LAT, SEQ), lambda g: (0, 0)),
        ],
        out_specs=[out_block, out_block],
        out_shape=[jax.ShapeDtypeStruct((LAT, LANE, LANE), F32)] * 2,
        compiler_params=pltpu.CompilerParams(vmem_limit_bytes=VMEM_ALL),
        cost_estimate=pl.CostEstimate(flops=18_000_000_000, bytes_accessed=70_000_000, transcendentals=0),
        name="weight_part",
    )(dkv, ct)


def late_kernel(p, other, with_rows, *refs):
    near, far = refs[0:3], refs[3:6]
    ct, wt, _, _, dc_in = refs[6:11]
    carry = ()
    if with_rows:
        o_in, dq_in, dwk, dwv, dc_out, o_out, dq_out, dc_acc, gbuf, wbuf, obuf, gsem, wsem, osem, o_buf, dq_buf, csem = refs[11:]
        carry = ((o_in, o_buf, o_out), (dq_in, dq_buf, dq_out))
    else:
        dwk, dwv, dc_out, dc_acc, gbuf, wbuf, obuf, gsem, wsem, osem = refs[11:]
    me = lax.axis_index("cp")
    src = flip(me, CORE) if other else me
    own = pl.ds(pl.multiple_of(me * TOK, TOK), TOK)
    tiles = [4 * p + place(flip(src, AZ * b)) // 4 for b in range(2)]
    for b in range(2):
        for i in range(2):
            for j in range(4):
                mask = AZ * b + 2 * j
                for k in range(3):
                    d = ORDERS[k][2]
                    ref, m = (far[k], mask - d) if mask & d else (near[k], mask)
                    pltpu.make_async_copy(ref.at[known(k, 2).index(m), pl.ds(i * ROWS[k][1], ROWS[k][1])],
                                          gbuf.at[b, i, j, pl.ds(ROWS[k][0], ROWS[k][1]), :], gsem.at[b, i]).start()
            pltpu.make_async_copy(wt.at[i, pl.ds(pl.multiple_of(tiles[b] * SUB, SUB), SUB)], wbuf.at[b, i], wsem.at[b, i]).start()
    if carry:
        moves = []
        for n, (src_ref, buf, dst_ref) in enumerate(carry):
            cp = pltpu.make_async_copy(src_ref, buf, csem.at[n])
            cp.start()
            moves.append((cp, pltpu.make_async_copy(buf, dst_ref, csem.at[n])))
    dc_acc[...] = dc_in[...]

    def store(b, i, tile):
        where = (dwk, dwv)[i].at[:, pl.ds(pl.multiple_of(tile * SUB, SUB), SUB), :]
        return pltpu.make_async_copy(obuf.at[b, i].reshape(LAT, SUB, LANE), where, osem.at[b, i])

    x, y = (src // AX) % 2, (src // AY) % 2

    def half_tile(n, carried):
        b, i = n // 2, n % 2
        pltpu.make_async_copy(gbuf.at[b, i], gbuf.at[b, i], gsem.at[b, i]).wait()
        pltpu.make_async_copy(wbuf.at[b, i], wbuf.at[b, i], wsem.at[b, i]).wait()
        for j in range(4):
            dx, dy = j % 2, j // 2
            slot = 2 * (2 * (y + dy - 2 * y * dy) + x + dx - 2 * x * dx)
            dc_acc[...] += dot_t(gbuf[b, i, j, own, :], jnp.concatenate([wbuf[b, i, slot], wbuf[b, i, slot + 1]], axis=-1))
            for m in range(2):
                res = dot(ct[m * WIDE:(m + 1) * WIDE, :], gbuf[b, i, j])
                for a in range(2):
                    obuf[b, i, pl.ds(m * 2048 + slot + a, WIDE, stride=SUB), :] = res[:, a * LANE:(a + 1) * LANE]
        tile = tiles[0] + b * (tiles[1] - tiles[0])
        for which in range(2):
            @pl.when(i == which)
            def _():
                store(b, which, tile).start()
        return carried

    lax.fori_loop(0, 4, half_tile, 0)
    dc_out[...] = dc_acc[...].astype(dc_out.dtype)
    if carry:
        for load, put in moves:
            load.wait()
            put.start()
        for load, put in moves:
            put.wait()
    for b in range(2):
        for i in range(2):
            store(b, i, tiles[b]).wait()


def late_part(p, other, last, near, far, ct, wt, dwk, dwv, dc, rows=()):
    any_spec = pl.BlockSpec(memory_space=pl.ANY)
    vmem = pl.BlockSpec(memory_space=pltpu.VMEM)
    dma = pltpu.SemaphoreType.DMA
    shapes = [jax.ShapeDtypeStruct(r.shape, r.dtype) for r in rows]
    return pl.pallas_call(
        functools.partial(late_kernel, p, other, bool(rows)),
        in_specs=[any_spec] * 6 + [vmem, any_spec, any_spec, any_spec, vmem] + [any_spec] * len(rows),
        out_specs=[any_spec, any_spec, vmem] + [any_spec] * len(rows),
        out_shape=[
            jax.ShapeDtypeStruct((LAT, LANE, LANE), F32),
            jax.ShapeDtypeStruct((LAT, LANE, LANE), F32),
            jax.ShapeDtypeStruct((TOK, LAT), BF16 if last else F32),
            *shapes,
        ],
        scratch_shapes=[
            pltpu.VMEM((TOK, LAT), F32),
            pltpu.VMEM((2, 2, 4, SEQ, WIDE), BF16),
            pltpu.VMEM((2, 2, SUB, LAT, LANE), BF16),
            pltpu.VMEM((2, 2, 4096, LANE), F32),
            dma((2, 2)), dma((2, 2)), dma((2, 2)),
            *([pltpu.VMEM(r.shape, r.dtype) for r in rows] + [dma((2,))] if rows else []),
        ],
        input_output_aliases={SUB: 0, 9: 1},
        compiler_params=pltpu.CompilerParams(vmem_limit_bytes=VMEM_ALL),
        cost_estimate=pl.CostEstimate(flops=4_500_000_000, bytes_accessed=20_000_000, transcendentals=0),
        name=f"late_part_{p}_{int(other)}",
    )(*near, *far, ct, wt, dwk, dwv, dc, *rows)


def solution(mesh):
    seq_spec = P("cp")

    def local_step(queries, latent, key_rope, w_uk, w_uv, d_out):
        scale = 1.0 / math.sqrt(queries.shape[-1])
        cr = jnp.concatenate([latent, key_rope, jnp.zeros_like(key_rope)], axis=-1)
        dkv, *late, wt, o, dq, dr, ct, dc = mega(scale, queries.transpose(0, 2, 1), d_out, cr, w_uk, w_uv)
        mine = {p: late[3 * i:3 * i + 3] for i, p in enumerate(LATE)}
        sibs = {p: late[6 + 3 * i:9 + 3 * i] for i, p in enumerate(LATE)}

        def swap(a, d):
            return lax.ppermute(a, "cp", [(i, i ^ d) for i in range(N_DEV)])

        far = {p: [swap(a, ORDERS[k][2]) for k, a in enumerate(mine[p])] for p in LATE}
        grads = (*weight_part(dkv, ct), dc)
        for p in LATE:
            got, grads = lax.optimization_barrier((far[p], grads))
            got_sib = [swap(a, CORE) for a in got]
            grads = late_part(p, False, False, mine[p], got, ct, wt, *grads)
            first = p == LATE[0]
            res = late_part(p, True, p == LATE[-1], sibs[p], got_sib, ct, wt, *grads, rows=(o, dq) if first else ())
            grads = res[:3]
            if first:
                o, dq = res[3:]
        dwk, dwv, dc = grads
        d_key_rope = (dr[:, :ROPE] + dr[:, ROPE:]).astype(BF16)
        return o, dq.transpose(0, 2, 1), dc, d_key_rope, dwk, dwv

    return jax.shard_map(local_step, mesh=mesh,
                         in_specs=(seq_spec, seq_spec, seq_spec, P(), P(), seq_spec),
                         out_specs=(seq_spec, seq_spec, seq_spec, seq_spec, P(), P()),
                         check_vma=False)
```

```python
import functools
import math
import jax
import jax.numpy as jnp
from jax import lax
from jax.experimental import pallas as pl
from jax.experimental.pallas import tpu as pltpu
from jax.sharding import PartitionSpec as P

N_DEV = 16
TOK = 64
SEQ = 1024
PAIRS = 64
OWN = 4
Q_BLK = 256
LANE = 128
WIDE = 256
LAT = 512
PACK = 640
ROPE = 64
SUB = 8
VMEM_ALL = 67_000_000
LOG2E = 1.4426950408889634
F32 = jnp.float32
BF16 = jnp.bfloat16
MESH = pl.DeviceIdType.MESH
CORE, AX, AY, AZ = 1, 2, 4, 8
ORDERS = ((AX, AY, AZ), (AY, AZ, AX), (AZ, AX, AY))
ROWS = ((0, 336), (336, 336), (672, 352))
BOTH = 2048
CHIPS = (0, 2, 4, 6, 8, 10, 12, 14)
UNITS = ((0, 0, 2), (1, 0, 2), (2, 0, 2), (3, 0, 2))
EARLY = 2
LATE = range(EARLY, len(UNITS))
PITCH = 136
PEERS = (14, 2, 4, 8, 15, 3, 5, 9, 6, 12, 10, 7, 13, 11, 1)


def dot(a, b):
    return lax.dot_general(a, b, (((1,), (0,)), ((), ())), preferred_element_type=F32)


def dot_t(a, b):
    return lax.dot_general(a, b, (((1,), (1,)), ((), ())), preferred_element_type=F32)


def flip(me, mask):
    out = me
    for bit in (1, 2, 4, SUB):
        if mask & bit:
            out = out + bit - 2 * bit * ((me // bit) % 2)
    return out


def place(dev):
    return (dev % 2) * SUB + dev // 2


def known(k, s):
    masks = [0]
    for d in ORDERS[k][:s]:
        masks = masks + [m + d for m in masks]
    return masks


def segments(which, lo, hi):
    parts = []
    for start, n in ROWS:
        a, b = max(lo, start), min(hi, start + n)
        if a < b:
            parts.append((a, b - a, start + which * n + a))
    return parts


def own_sixteen(me, n, which):
    sixteen = 4 * me + n
    third = sixteen // 21 - sixteen // 63
    return pl.multiple_of(N_DEV * (sixteen + 21 * third + which * (21 + third // 2)), N_DEV)


def head_pair(scale, x, c, ropes, wk, wv, out, dr_ref, kx_ref, v_ref, q_ref, p_ref, ds_ref):
    n_blk = SEQ // Q_BLK
    scale2 = scale * LOG2E
    k_all = dot(c, wk).astype(BF16)
    v_ref[...] = dot(c, wv).astype(BF16)
    lane = lax.broadcasted_iota(jnp.int32, (Q_BLK, LANE), 1)
    key = lax.broadcasted_iota(jnp.int32, (Q_BLK, Q_BLK), 0)
    qry = lax.broadcasted_iota(jnp.int32, (Q_BLK, Q_BLK), 1)
    for a in range(2):
        cols = slice(a * LANE, (a + 1) * LANE)
        kx_ref[...] = jnp.concatenate([k_all[:, cols], ropes[a]], axis=-1)
        q_ref[...] = jnp.concatenate([x[:, cols], x[:, LAT:PACK]], axis=-1)
        do = x[:, WIDE + a * LANE:384 + a * LANE]
        for i in range(n_blk):
            top = (i + 1) * Q_BLK
            rows = slice(i * Q_BLK, top)
            s = dot_t(kx_ref[:top, :], q_ref[rows, :]) * scale2
            diag = jnp.where(key <= qry, s[i * Q_BLK:, :], -1e30)
            s = diag if i == 0 else jnp.concatenate([s[:i * Q_BLK, :], diag], axis=0)
            e = jnp.exp2(s - jnp.max(s, axis=0, keepdims=True))
            p = e * (1.0 / jnp.sum(e, axis=0, keepdims=True))
            dp = dot_t(v_ref[:top, cols], do[rows, :])
            delta = jnp.sum(p * dp, axis=0, keepdims=True)
            p_ref[:top, rows] = p.astype(BF16)
            ds_ref[:top, rows] = (p * (dp - delta)).astype(BF16)
        for j in range(n_blk):
            rows = slice(j * Q_BLK, (j + 1) * Q_BLK)
            dv = dot(p_ref[rows, j * Q_BLK:], do[j * Q_BLK:, :]).astype(BF16)
            dk = dot(ds_ref[rows, j * Q_BLK:], q_ref[j * Q_BLK:, :]) * scale
            for which, grad in enumerate((dk[:, :LANE].astype(BF16), dv)):
                for row, n, at in segments(which, j * Q_BLK, (j + 1) * Q_BLK):
                    out[at:at + n, cols] = grad[row - j * Q_BLK:row - j * Q_BLK + n, :]
            keep = lane < ROPE if a == 0 else lane >= ROPE
            dr_ref[rows, :] = dr_ref[rows, :] + jnp.where(keep, dk[:, LANE:], 0.0)


def query_pair(scale, me, x, k_all, v_all, r):
    scale2 = scale * LOG2E
    z = jnp.zeros((TOK, LANE), BF16)

    def diagonal(u):
        return jnp.concatenate([jnp.concatenate([u[:, :LANE], z], axis=1), jnp.concatenate([z, u[:, LANE:]], axis=1)], axis=0)

    q_rope = jnp.concatenate([x[:, LAT:576], x[:, 576:PACK]], axis=0)
    s = (dot_t(k_all, diagonal(x[:, :WIDE])) + dot_t(r[:, :ROPE], q_rope)) * scale2
    key = lax.broadcasted_iota(jnp.int32, (SEQ, LANE), 0)
    qry = lax.broadcasted_iota(jnp.int32, (SEQ, LANE), 1) % TOK + me * TOK
    s = jnp.where(key <= qry, s, -1e30)
    e = jnp.exp2(s - jnp.max(s, axis=0, keepdims=True))
    p = e * (1.0 / jnp.sum(e, axis=0, keepdims=True))
    dp = dot_t(v_all, diagonal(x[:, WIDE:LAT]))
    ds = (p * (dp - jnp.sum(p * dp, axis=0, keepdims=True))).astype(BF16).T
    o = dot(p.astype(BF16).T, v_all)
    dq = dot(ds, k_all) * scale
    dq_rope = dot(ds, r) * scale
    halves = (slice(0, TOK), slice(TOK, 2 * TOK))
    return [(o[h, c], dq[h, c], dq_rope[h, :]) for h, c in zip(halves, (slice(0, LANE), slice(LANE, WIDE)))]


def mega_kernel(scale, *refs):
    q_in, do_in, cr, wk, wv, dkv = refs[:6]
    n_late = 3 * len(LATE)
    late = {u: refs[6 + 3 * i:9 + 3 * i] for i, u in enumerate(LATE)}
    late_sib = {u: refs[6 + n_late + 3 * i:9 + n_late + 3 * i] for i, u in enumerate(LATE)}
    mega_body(scale, late, late_sib, q_in, do_in, cr, wk, wv, dkv, *refs[6 + 2 * n_late:])


def mega_body(scale, late, late_sib, q_in, do_in, cr, wk, wv, dkv, wt_out, o_out, dq_out, dr_out, ct_out, dc_out,
              xbuf, cbuf, rb, wnat, wt, wt_own, kv, stage, kx, vs, qs, ps, dss, dr_acc, dr_land, pay, grow, osc, dqn, dqr, dos,
                c_send, c_recv, c_sib, x_send, x_recv, ici_send, ici_recv, sib_send, sib_recv,
                dr_send, dr_recv, load_sem, own_sem, wsem, xq_sem, wt_sem, st_sem):
    me = lax.axis_index("cp")
    core = me % 2
    chip = me // 2
    sib = flip(me, CORE)
    by_token = [pltpu.make_async_copy(src, dst, own_sem.at[n]) for n, (src, dst) in enumerate(((q_in, dq_out), (do_in, o_out)))]
    for cp in by_token:
        cp.start()
    bar = pltpu.get_barrier_semaphore()
    for m in range(1, N_DEV):
        pl.semaphore_signal(bar, inc=1, device_id=(flip(me, m),), device_id_type=MESH)
    pl.semaphore_wait(bar, N_DEV - 1)

    def remote(src, dst, ssem, rsem, to):
        return pltpu.make_async_remote_copy(src_ref=src, dst_ref=dst, send_sem=ssem, recv_sem=rsem,
                                            device_id=(to,), device_id_type=MESH)

    for m in CHIPS[1:]:
        remote(cr, cbuf.at[chip, core], c_send, c_recv, flip(me, m)).start()
    own_c = pltpu.make_async_copy(cr, cbuf.at[chip, core], load_sem.at[0])
    own_c.start()

    def fetch_tile(tile, slot):
        return [pltpu.make_async_copy(w.at[:, pl.ds(pl.multiple_of(tile * SUB, SUB), SUB), :], wnat.at[slot, i], wsem.at[slot, i])
                for i, w in enumerate((wk, wv))]

    def own_tile(pp):
        return 4 * pp + place(me) // 4

    for pp in range(2):
        for cp in fetch_tile(own_tile(pp), pp):
            cp.start()
    for cp in by_token:
        cp.wait()

    def unpack_token(t, carry):
        rows = pl.ds(pl.multiple_of(t * PITCH, SUB), LANE)
        qt = dq_out[t].astype(F32)
        dqn[rows, :] = qt[:LANE, :].T
        dqr[rows, 0:ROPE] = qt[LANE:, :].T
        dos[rows, :] = o_out[t].astype(F32)
        return carry

    lax.fori_loop(0, TOK, unpack_token, 0, unroll=SUB)

    def pack_pair(p, carry):
        rope = []
        for a in range(2):
            rows = pl.ds(2 * p + a, TOK, stride=PITCH)
            pay[p, :, a * LANE:(a + 1) * LANE] = dqn[rows, :].astype(BF16)
            pay[p, :, (a + 2) * LANE:(a + 3) * LANE] = dos[rows, :].astype(BF16)
            rope.append(dqr[rows, :][:, :ROPE])
        pay[p, :, LAT:] = jnp.concatenate(rope, axis=-1).astype(BF16)
        return carry

    def to_owners(pp):
        for m in PEERS:
            to = flip(me, m)
            remote(pay.at[N_DEV * pp + place(to)], xbuf.at[pp, me], x_send, x_recv.at[pp], to).start()

    for pp in range(OWN):
        lax.fori_loop(N_DEV * pp, N_DEV * (pp + 1), pack_pair, 0, unroll=4)
        if pp:
            to_owners(pp - 1)

    dr_acc[...] = jnp.zeros_like(dr_acc)
    first = 2 * (place(me) % 4)
    for pp in range(OWN):
        for cp in fetch_tile(own_tile(pp), pp % 2):
            cp.wait()
        for i in range(2):
            wt[pp % 2, i] = jnp.transpose(wnat[pp % 2, i], (1, 0, 2))
            wt_own[pp, i] = wt[pp % 2, i, pl.ds(first, 2)]
        for cp in fetch_tile(own_tile(pp + 2), pp) if pp < 2 else fetch_tile(pp - 2, pp - 2):
            cp.start()
        if pp == 0:
            to_owners(OWN - 1)
    own_c.wait()
    arrived = cbuf.at[pl.ds(0, 7), 0]
    pltpu.make_async_copy(arrived, arrived, c_recv).wait()
    fwd = remote(cbuf.at[:, core], cbuf.at[:, core], c_send, c_sib, sib)
    fwd.start()
    fwd.wait_recv()

    def latent():
        return cbuf[...].reshape(SEQ, PACK)

    rope_a = latent()[:, LAT:PACK].astype(F32)
    rb[...] = pltpu.roll(rope_a, ROPE, axis=1).astype(BF16)

    def operands():
        cc = latent()
        return cc[:, :LAT], (cc[:, LAT:PACK], rb[...])

    for pp in range(OWN):
        xbuf[pp, me] = pay[N_DEV * pp + place(me)]

    def block(mask, p, k):
        if p in LATE:
            return late[p][k].at[known(k, 2).index(mask)]
        return dkv.at[N_DEV * p + place(flip(me, mask)), pl.ds(2 * ROWS[k][0], 2 * ROWS[k][1]), :]

    def to_sibling(mask, p, k):
        b = block(mask, p, k)
        there = late_sib[p][k].at[known(k, 2).index(mask)] if p in LATE else b
        remote(b, there, sib_send, sib_recv.at[p], sib).start()

    def gather_stage(p, s):
        last = 2 if p in LATE else 3
        fresh = [[0] if s == 0 else [m + ORDERS[k][s - 1] for m in known(k, s - 1)] for k in range(3)]

        def arrive(k, m):
            b = block(m, p, k)
            pltpu.make_async_copy(b, b, ici_recv.at[p, k, m // 2]).wait()

        if s == last:
            for j in range(len(fresh[0])):
                for k in range(3):
                    arrive(k, fresh[k][j])
                    to_sibling(fresh[k][j], p, k)
            return
        for k in range(3):
            if s > 0:
                for m in fresh[k]:
                    arrive(k, m)
            d = ORDERS[k][s]
            for m in known(k, s):
                there = block(m + d, p, k) if p in LATE else block(m, p, k)
                remote(block(m, p, k), there, ici_send, ici_recv.at[p, k, (m + d) // 2], flip(me, d)).start()
        for k in range(3):
            for m in fresh[k]:
                to_sibling(m, p, k)

    def head_step(pp):
        got = xbuf.at[pp, pl.ds(0, N_DEV - 1)]
        pltpu.make_async_copy(got, got, x_recv.at[pp]).wait()
        x = xbuf[pp].reshape(SEQ, PACK)
        c, ropes = operands()
        wkp = jnp.concatenate([wt_own[pp, 0, 0], wt_own[pp, 0, 1]], axis=-1)
        wvp = jnp.concatenate([wt_own[pp, 1, 0], wt_own[pp, 1, 1]], axis=-1)
        head_pair(scale, x, c, ropes, wkp, wvp, stage, dr_acc, kx, vs, qs, ps, dss)

        for p in range(OWN):
            @pl.when(pp == p)
            def _():
                cps = []
                for u, (pair, kind, n_kind) in enumerate(UNITS):
                    if pair != p:
                        continue
                    if u in LATE:
                        for k, (start, n) in enumerate(ROWS):
                            cps.append(pltpu.make_async_copy(
                                stage.at[pl.ds(2 * start + kind * n, n_kind * n), :], late[u][k].at[0], st_sem.at[3 * kind + k]))
                    else:
                        cps.append(pltpu.make_async_copy(stage, dkv.at[N_DEV * p + place(me)], st_sem.at[0]))
                for cp in cps:
                    cp.start()
                for cp in cps:
                    cp.wait()
                for u, unit in enumerate(UNITS):
                    if unit[0] == p:
                        gather_stage(u, 0)

    own_dr = pltpu.make_async_copy(dr_acc.at[pl.ds(pl.multiple_of(me * TOK, TOK), TOK), :], dr_out, load_sem.at[1])

    def share_rope():
        for m in range(1, N_DEV):
            to = flip(me, m)
            remote(dr_acc.at[pl.ds(pl.multiple_of(to * TOK, TOK), TOK), :], dr_land.at[me], dr_send, dr_recv, to).start()
        own_dr.start()

    def put_w(g, slot):
        return pltpu.make_async_copy(wt.at[slot], wt_out.at[:, pl.ds(pl.multiple_of(g * SUB, SUB), SUB)], wt_sem.at[slot])

    plan = {4: ((0, 1),), 5: ((1, 1),), 9: ((0, 2),), 10: ((1, 2),), 13: ((2, 1),), 15: tuple((u, 1) for u in LATE[1:])}

    def query_step(g, carry):
        slot = g % 2
        for cp in fetch_tile(g, slot):
            cp.wait()

        @pl.when((g > 0) & (g < 15))
        def _():
            for cp in fetch_tile(g + 1, 1 - slot):
                cp.start()

        @pl.when(g >= 2)
        def _():
            put_w(g - 2, slot).wait()

        for i in range(2):
            wt[slot, i] = jnp.transpose(wnat[slot, i], (1, 0, 2))
        put_w(g, slot).start()

        def project(j):
            c = latent()[:, :LAT]
            for i in range(2):
                kv[j % 2, i] = dot(c, jnp.concatenate([wt[slot, i, 2 * j], wt[slot, i, 2 * j + 1]], axis=-1)).astype(BF16)

        project(0)
        for j in range(4):
            if j < 3:
                project(j + 1)
            r = latent()[:, LAT:PACK]
            res = query_pair(scale, me, pay[4 * g + j], kv[j % 2, 0], kv[j % 2, 1], r)
            for a in range(2):
                o, dq, dq_rope = res[a]
                osc[pl.ds(2 * j + a, TOK, stride=SUB), :] = o
                rows = pl.ds(g * SUB + 2 * j + a, TOK, stride=PITCH)
                dqn[rows, :] = dq
                dqr[rows, :] = dq_rope
        o_out[:, pl.ds(pl.multiple_of(g * SUB, SUB), SUB), :] = osc[...].reshape(TOK, SUB, LANE).astype(BF16)

        @pl.when(g < OWN)
        def _():
            head_step(g)

        @pl.when(g == OWN - 1)
        def _():
            share_rope()

        for when, events in plan.items():
            @pl.when(g == when)
            def _():
                for p, s in events:
                    gather_stage(p, s)
        return carry

    lax.fori_loop(0, 16, query_step, 0)

    def dq_token(t, carry):
        rows = pl.ds(pl.multiple_of(t * PITCH, SUB), LANE)
        dq_out[t, 0:LANE, :] = dqn[rows, :].T.astype(BF16)
        dq_out[t, LANE:192, :] = dqr[rows, :].T[0:ROPE, :].astype(BF16)
        return carry

    lax.fori_loop(0, TOK, dq_token, 0)
    ct_out[...] = latent()[:, :LAT].T
    put_w(14, 0).wait()
    put_w(15, 1).wait()
    for p in range(EARLY):
        gather_stage(p, 3)
    for p in range(EARLY):
        got = dkv.at[pl.ds(N_DEV * p, SUB)]
        pltpu.make_async_copy(got, got, sib_recv.at[p]).wait()

    def rows_of(t, slot):
        cps = [pltpu.make_async_copy(wt_out.at[:, pl.ds(pl.multiple_of(t * SUB, SUB), SUB)], wt.at[slot], wt_sem.at[slot])]
        for n in range(4):
            for i in range(2):
                at = pl.ds(own_sixteen(me, n, i), N_DEV)
                cps.append(pltpu.make_async_copy(dkv.at[pl.ds(4 * t, 4), at, :],
                                                 grow.at[slot, i, :, pl.ds(N_DEV * n, N_DEV), :], xq_sem.at[slot, 4 * i + n]))
        return cps

    for cp in rows_of(0, 0):
        cp.start()
    dc_out[...] = jnp.zeros_like(dc_out)

    def dc_step(t, carry):
        slot = t % 2
        for cp in rows_of(t, slot):
            cp.wait()

        @pl.when(t < SUB - 1)
        def _():
            for cp in rows_of(t + 1, 1 - slot):
                cp.start()

        for i in range(2):
            for j in range(4):
                w = jnp.concatenate([wt[slot, i, 2 * j], wt[slot, i, 2 * j + 1]], axis=-1)
                dc_out[...] += dot_t(grow[slot, i, j], w)
        return carry

    lax.fori_loop(0, SUB, dc_step, 0)
    for p in LATE:
        gather_stage(p, 2)

    own_dr.wait()
    got = dr_land.at[pl.ds(0, N_DEV - 1)]
    pltpu.make_async_copy(got, got, dr_recv).wait()
    total = dr_out[...]
    for m in range(1, N_DEV):
        total = total + dr_land[flip(me, m)]
    dr_out[...] = total

    pltpu.make_async_copy(got, got, dr_send).wait()
    got = xbuf.at[:, pl.ds(0, N_DEV - 1)]
    pltpu.make_async_copy(got, got, x_send).wait()
    arrived = cbuf.at[pl.ds(0, 7), 0]
    pltpu.make_async_copy(arrived, arrived, c_send).wait()
    arrived = cbuf.at[:, 0]
    pltpu.make_async_copy(arrived, arrived, c_send).wait()
    sent = dkv.at[pl.ds(0, 20)]
    pltpu.make_async_copy(sent, sent, ici_send).wait()
    sent = dkv.at[pl.ds(0, 24)]
    pltpu.make_async_copy(sent, sent, sib_send).wait()
    for p in LATE:
        got = dkv.at[pl.ds(0, 2 * UNITS[p][2])]
        pltpu.make_async_copy(got, got, sib_recv.at[p]).wait()


def mega(scale, q_t, d_out, cr, wk, wv):
    any_spec = pl.BlockSpec(memory_space=pl.ANY)
    vmem = pl.BlockSpec(memory_space=pltpu.VMEM)
    dma = pltpu.SemaphoreType.DMA
    return pl.pallas_call(
        functools.partial(mega_kernel, scale),
        in_specs=[any_spec] * 5,
        out_specs=[any_spec] * (2 + 6 * len(LATE)) + [vmem] * 5,
        out_shape=[
            jax.ShapeDtypeStruct((32, BOTH, WIDE), BF16),
            *[jax.ShapeDtypeStruct((4, UNITS[u][2] * n, WIDE), BF16) for _ in range(2) for u in LATE for _, n in ROWS],
            jax.ShapeDtypeStruct((2, LANE, LAT, LANE), BF16),
            jax.ShapeDtypeStruct((TOK, LANE, LANE), BF16),
            jax.ShapeDtypeStruct((TOK, 192, LANE), BF16),
            jax.ShapeDtypeStruct((TOK, LANE), F32),
            jax.ShapeDtypeStruct((LAT, SEQ), BF16),
            jax.ShapeDtypeStruct((TOK, LAT), F32),
        ],
        scratch_shapes=[
            pltpu.VMEM((OWN, N_DEV, TOK, PACK), BF16),
            pltpu.VMEM((SUB, 2, TOK, PACK), BF16),
            pltpu.VMEM((SEQ, LANE), BF16),
            pltpu.VMEM((2, 2, LAT, SUB, LANE), BF16),
            pltpu.VMEM((2, 2, SUB, LAT, LANE), BF16),
            pltpu.VMEM((OWN, 2, 2, LAT, LANE), BF16),
            pltpu.VMEM((2, 2, SEQ, WIDE), BF16),
            pltpu.VMEM((BOTH, WIDE), BF16),
            pltpu.VMEM((SEQ, WIDE), BF16), pltpu.VMEM((SEQ, WIDE), BF16), pltpu.VMEM((SEQ, WIDE), BF16),
            pltpu.VMEM((SEQ, SEQ), BF16), pltpu.VMEM((SEQ, SEQ), BF16),
            pltpu.VMEM((SEQ, LANE), F32),
            pltpu.VMEM((N_DEV, TOK, LANE), F32),
            pltpu.VMEM((PAIRS, TOK, PACK), BF16),
            pltpu.VMEM((2, 2, 4, TOK, WIDE), BF16),
            pltpu.VMEM((TOK * SUB, LANE), F32),
            *[pltpu.VMEM((TOK * PITCH, LANE), F32)] * 3,
            dma, dma, dma, dma, dma((OWN,)), dma, dma((len(UNITS), 3, SUB)), dma, dma((len(UNITS),)),
            dma, dma, dma((2,)), dma((2,)), dma((2, 2)), dma((2, SUB)), dma((2,)), dma((6,)),
        ],
        compiler_params=pltpu.CompilerParams(collective_id=0, has_side_effects=True, vmem_limit_bytes=VMEM_ALL),
        cost_estimate=pl.CostEstimate(flops=100_000_000_000, bytes_accessed=200_000_000, transcendentals=0),
        name="mega",
    )(q_t, d_out, cr, wk, wv)


def weight_kernel(dkv_ref, ct_ref, dwk_ref, dwv_ref):
    for which, out_ref in enumerate((dwk_ref, dwv_ref)):
        flat = out_ref.reshape(LAT * SUB, LANE)
        for p in range(4):
            g = jnp.concatenate([dkv_ref[p, at:at + n, :] for _, n, at in segments(which, 0, SEQ)], axis=0)
            for m in range(2):
                res = dot(ct_ref[m * WIDE:(m + 1) * WIDE, :], g)
                for a in range(2):
                    flat[pl.ds(m * BOTH + 2 * p + a, WIDE, stride=SUB), :] = res[:, a * LANE:(a + 1) * LANE]


def weight_part(dkv, ct):
    out_block = pl.BlockSpec((LAT, SUB, LANE), lambda g: (0, g, 0))
    return pl.pallas_call(
        weight_kernel,
        grid=(SUB,),
        in_specs=[
            pl.BlockSpec((4, BOTH, WIDE), lambda g: (g, 0, 0)),
            pl.BlockSpec((LAT, SEQ), lambda g: (0, 0)),
        ],
        out_specs=[out_block, out_block],
        out_shape=[jax.ShapeDtypeStruct((LAT, LANE, LANE), F32)] * 2,
        compiler_params=pltpu.CompilerParams(vmem_limit_bytes=VMEM_ALL),
        cost_estimate=pl.CostEstimate(flops=18_000_000_000, bytes_accessed=70_000_000, transcendentals=0),
        name="weight_part",
    )(dkv, ct)


def late_kernel(unit, other, with_rows, *refs):
    pair, kind, n_kind = unit
    near, far = refs[0:3], refs[3:6]
    ct_in, wt, dc_in = refs[6:9]
    refs = refs[9 + n_kind:]
    rows_in, refs = (refs[:2], refs[2:]) if with_rows else ((), refs)
    grads, dc_out, refs = refs[:n_kind], refs[n_kind], refs[n_kind + 1:]
    rows_out, refs = (refs[:2], refs[2:]) if with_rows else ((), refs)
    ct, dc_buf, dc_last, gbuf, wbuf, obuf, ct_sem, gsem, wsem, osem = refs[:10]
    refs = refs[10:]
    me = lax.axis_index("cp")
    src = flip(me, CORE) if other else me
    own = pl.ds(pl.multiple_of(me * TOK, TOK), TOK)
    tiles = [4 * pair + place(flip(src, AZ * b)) // 4 for b in range(2)]
    load_ct = pltpu.make_async_copy(ct_in, ct, ct_sem.at[0])
    load_dc = pltpu.make_async_copy(dc_in, dc_buf, ct_sem.at[1])

    def fetch(n):
        b, i = n // n_kind, n % n_kind
        for j in range(4):
            mask = AZ * b + 2 * j
            for k, (start, n_row) in enumerate(ROWS):
                d = ORDERS[k][2]
                ref, m = (far[k], mask - d) if mask & d else (near[k], mask)
                pltpu.make_async_copy(ref.at[known(k, 2).index(m), pl.ds(i * n_row, n_row)],
                                      gbuf.at[b, i, j, pl.ds(start, n_row), :], gsem.at[b, i]).start()
        pltpu.make_async_copy(wt.at[kind + i, pl.ds(pl.multiple_of(tiles[b] * SUB, SUB), SUB)], wbuf.at[b, i], wsem.at[b, i]).start()

    fetch(0)
    load_ct.start()
    load_dc.start()
    fetch(1)
    moves = []
    for n in range(len(rows_in)):
        moves.append((pltpu.make_async_copy(rows_in[n], refs[n], refs[-1].at[n]),
                      pltpu.make_async_copy(refs[n], rows_out[n], refs[-1].at[n])))
        moves[-1][0].start()

    def store(b, i, tile):
        where = grads[i].at[:, pl.ds(pl.multiple_of(tile * SUB, SUB), SUB), :]
        return pltpu.make_async_copy(obuf.at[b, i].reshape(LAT, SUB, LANE), where, osem.at[b, i])

    x, y = (src // AX) % 2, (src // AY) % 2
    load_ct.wait()
    load_dc.wait()

    def half_tile(n, carried):
        b, i = n // n_kind, n % n_kind
        tile = tiles[0] + b * (tiles[1] - tiles[0])
        slots = []
        for j in range(4):
            dx, dy = j % 2, j // 2
            slots.append(2 * (2 * (y + dy - 2 * y * dy) + x + dx - 2 * x * dx))
        for buf, sem in ((gbuf, gsem), (wbuf, wsem)):
            pltpu.make_async_copy(buf.at[b, i], buf.at[b, i], sem.at[b, i]).wait()
        for later in range(2, 2 * n_kind):
            @pl.when(n == later - 2)
            def _():
                fetch(later)
        dc = dc_buf[...]
        for j in range(4):
            dc += dot_t(gbuf[b, i, j, own, :], jnp.concatenate([wbuf[b, i, slots[j]], wbuf[b, i, slots[j] + 1]], axis=-1))
            for m in range(2):
                res = dot(ct[m * WIDE:(m + 1) * WIDE, :], gbuf[b, i, j])
                for a in range(2):
                    obuf[b, i, pl.ds(m * BOTH + slots[j] + a, WIDE, stride=SUB), :] = res[:, a * LANE:(a + 1) * LANE]
        dc_buf[...] = dc
        for which in range(n_kind):
            @pl.when(i == which)
            def _():
                store(b, which, tile).start()
        return carried

    lax.fori_loop(0, 2 * n_kind, half_tile, 0)
    dc_last[...] = dc_buf[...].astype(dc_last.dtype)
    put_dc = pltpu.make_async_copy(dc_last, dc_out, ct_sem.at[0])
    put_dc.start()
    for load, put in moves:
        load.wait()
        put.start()
    for load, put in moves:
        put.wait()
    for b in range(2):
        for i in range(n_kind):
            store(b, i, tiles[b]).wait()
    put_dc.wait()


def late_part(unit, other, near, far, ct, wt, dc, grads, dc_type, rows=()):
    n_kind = unit[2]
    any_spec = pl.BlockSpec(memory_space=pl.ANY)
    dma = pltpu.SemaphoreType.DMA
    like = lambda arrays: [jax.ShapeDtypeStruct(r.shape, r.dtype) for r in arrays]
    res = pl.pallas_call(
        functools.partial(late_kernel, unit, other, bool(rows)),
        in_specs=[any_spec] * (9 + n_kind + len(rows)),
        out_specs=[any_spec] * (n_kind + 1 + len(rows)),
        out_shape=like(grads) + [jax.ShapeDtypeStruct(dc.shape, dc_type)] + like(rows),
        scratch_shapes=[
            pltpu.VMEM((LAT, SEQ), BF16), pltpu.VMEM(dc.shape, F32), pltpu.VMEM(dc.shape, dc_type),
            pltpu.VMEM((2, n_kind, 4, SEQ, WIDE), BF16),
            pltpu.VMEM((2, n_kind, SUB, LAT, LANE), BF16),
            pltpu.VMEM((2, n_kind, 2 * BOTH, LANE), F32),
            dma((2,)), dma((2, n_kind)), dma((2, n_kind)), dma((2, n_kind)),
            *([pltpu.VMEM(r.shape, r.dtype) for r in rows] + [dma((2,))] if rows else []),
        ],
        input_output_aliases={9 + n: n for n in range(n_kind)},
        compiler_params=pltpu.CompilerParams(vmem_limit_bytes=VMEM_ALL),
        cost_estimate=pl.CostEstimate(flops=2_200_000_000 * n_kind, bytes_accessed=10_000_000 * n_kind, transcendentals=0),
        name="late_part",
    )(*near, *far, ct, wt, dc, *grads, *rows)
    return res[:n_kind], res[n_kind], res[n_kind + 1:]


def solution(mesh):
    seq_spec = P("cp")

    def local_step(queries, latent, key_rope, w_uk, w_uv, d_out):
        scale = 1.0 / math.sqrt(queries.shape[-1])
        cr = jnp.concatenate([latent, key_rope, jnp.zeros_like(key_rope)], axis=-1)
        dkv, *late, wt, o, dq, dr, ct, dc = mega(scale, queries.transpose(0, 2, 1), d_out, cr, w_uk, w_uv)
        mine = {u: late[3 * i:3 * i + 3] for i, u in enumerate(LATE)}
        sibs = {u: late[3 * (i + len(LATE)):][:3] for i, u in enumerate(LATE)}

        def swap(a, d):
            return lax.ppermute(a, "cp", [(i, i ^ d) for i in range(N_DEV)])

        far = {}
        for u in LATE:
            far[u] = [swap(a, ORDERS[k][2]) for k, a in enumerate(mine[u])]
        grads = list(weight_part(dkv, ct))
        for u in LATE:
            got, grads, dc = lax.optimization_barrier((far[u], grads, dc))
            got_sib = [swap(a, CORE) for a in got]
            _, kind, n_kind = UNITS[u]
            for other, near, here in ((False, mine[u], got), (True, sibs[u], got_sib)):
                rows = (o, dq) if other and u == EARLY else ()
                grads[kind:kind + n_kind], dc, rows = late_part(
                    UNITS[u], other, near, here, ct, wt, dc, grads[kind:kind + n_kind],
                    BF16 if other and u == LATE[-1] else F32, rows)
                if rows:
                    o, dq = rows
        dwk, dwv = grads
        d_key_rope = (dr[:, :ROPE] + dr[:, ROPE:]).astype(BF16)
        return o, dq.transpose(0, 2, 1), dc, d_key_rope, dwk, dwv

    return jax.shard_map(local_step, mesh=mesh,
                         in_specs=(seq_spec, seq_spec, seq_spec, P(), P(), seq_spec),
                         out_specs=(seq_spec, seq_spec, seq_spec, seq_spec, P(), P()),
                         check_vma=False)
```

```python
import functools
import math
import jax
import jax.numpy as jnp
from jax import lax
from jax.experimental import pallas as pl
from jax.experimental.pallas import tpu as pltpu
from jax.sharding import PartitionSpec as P

N_DEV = 16
TOK = 64
SEQ = 1024
PAIRS = 64
OWN = 4
Q_BLK = 256
LANE = 128
WIDE = 256
LAT = 512
PACK = 640
ROPE = 64
SUB = 8
VMEM_ALL = 67_000_000
LOG2E = 1.4426950408889634
F32 = jnp.float32
BF16 = jnp.bfloat16
MESH = pl.DeviceIdType.MESH
CORE, AX, AY, AZ = 1, 2, 4, 8
ORDERS = ((AX, AY, AZ), (AY, AZ, AX), (AZ, AX, AY))
ROWS = ((0, 336), (336, 336), (672, 352))
BOTH = 2048
CHIPS = (0, 2, 4, 6, 8, 10, 12, 14)
UNITS = ((0, 0, 2), (1, 0, 2), (2, 0, 2), (3, 0, 2))
EARLY = 2
LATE = range(EARLY, len(UNITS))
HANDED = LATE[:-1]
PITCH = 136
PEERS = (2, 4, 8, 6, 12, 10, 14, 3, 5, 9, 7, 13, 11, 15, 1)


def dot(a, b):
    return lax.dot_general(a, b, (((1,), (0,)), ((), ())), preferred_element_type=F32)


def dot_t(a, b):
    return lax.dot_general(a, b, (((1,), (1,)), ((), ())), preferred_element_type=F32)


def flip(me, mask):
    out = me
    for bit in (1, 2, 4, SUB):
        if mask & bit:
            out = out + bit - 2 * bit * ((me // bit) % 2)
    return out


def place(dev):
    return (dev % 2) * SUB + dev // 2


def known(k, s):
    masks = [0]
    for d in ORDERS[k][:s]:
        masks = masks + [m + d for m in masks]
    return masks


def segments(which, lo, hi):
    parts = []
    for start, n in ROWS:
        a, b = max(lo, start), min(hi, start + n)
        if a < b:
            parts.append((a, b - a, start + which * n + a))
    return parts


def own_sixteen(me, n, which):
    sixteen = 4 * me + n
    third = sixteen // 21 - sixteen // 63
    return pl.multiple_of(N_DEV * (sixteen + 21 * third + which * (21 + third // 2)), N_DEV)


def head_pair(scale, x, c, ropes, wk, wv, out, dr_ref, kx_ref, v_ref, q_ref, p_ref, ds_ref):
    n_blk = SEQ // Q_BLK
    scale2 = scale * LOG2E
    k_all = dot(c, wk).astype(BF16)
    v_ref[...] = dot(c, wv).astype(BF16)
    lane = lax.broadcasted_iota(jnp.int32, (Q_BLK, LANE), 1)
    key = lax.broadcasted_iota(jnp.int32, (Q_BLK, Q_BLK), 0)
    qry = lax.broadcasted_iota(jnp.int32, (Q_BLK, Q_BLK), 1)
    for a in range(2):
        cols = slice(a * LANE, (a + 1) * LANE)
        kx_ref[...] = jnp.concatenate([k_all[:, cols], ropes[a]], axis=-1)
        q_ref[...] = jnp.concatenate([x[:, cols], x[:, LAT:PACK]], axis=-1)
        do = x[:, WIDE + a * LANE:384 + a * LANE]
        for i in range(n_blk):
            top = (i + 1) * Q_BLK
            rows = slice(i * Q_BLK, top)
            s = dot_t(kx_ref[:top, :], q_ref[rows, :]) * scale2
            diag = jnp.where(key <= qry, s[i * Q_BLK:, :], -1e30)
            s = diag if i == 0 else jnp.concatenate([s[:i * Q_BLK, :], diag], axis=0)
            e = jnp.exp2(s - jnp.max(s, axis=0, keepdims=True))
            p = e * (1.0 / jnp.sum(e, axis=0, keepdims=True))
            dp = dot_t(v_ref[:top, cols], do[rows, :])
            delta = jnp.sum(p * dp, axis=0, keepdims=True)
            p_ref[:top, rows] = p.astype(BF16)
            ds_ref[:top, rows] = (p * (dp - delta)).astype(BF16)
        for j in range(n_blk):
            rows = slice(j * Q_BLK, (j + 1) * Q_BLK)
            dv = dot(p_ref[rows, j * Q_BLK:], do[j * Q_BLK:, :]).astype(BF16)
            dk = dot(ds_ref[rows, j * Q_BLK:], q_ref[j * Q_BLK:, :]) * scale
            for which, grad in enumerate((dk[:, :LANE].astype(BF16), dv)):
                for row, n, at in segments(which, j * Q_BLK, (j + 1) * Q_BLK):
                    out[at:at + n, cols] = grad[row - j * Q_BLK:row - j * Q_BLK + n, :]
            keep = lane < ROPE if a == 0 else lane >= ROPE
            dr_ref[rows, :] = dr_ref[rows, :] + jnp.where(keep, dk[:, LANE:], 0.0)


def query_pair(scale, me, x, k_all, v_all, r):
    scale2 = scale * LOG2E
    z = jnp.zeros((TOK, LANE), BF16)

    def diagonal(u):
        return jnp.concatenate([jnp.concatenate([u[:, :LANE], z], axis=1), jnp.concatenate([z, u[:, LANE:]], axis=1)], axis=0)

    q_rope = jnp.concatenate([x[:, LAT:576], x[:, 576:PACK]], axis=0)
    s = (dot_t(k_all, diagonal(x[:, :WIDE])) + dot_t(r[:, :ROPE], q_rope)) * scale2
    key = lax.broadcasted_iota(jnp.int32, (SEQ, LANE), 0)
    qry = lax.broadcasted_iota(jnp.int32, (SEQ, LANE), 1) % TOK + me * TOK
    s = jnp.where(key <= qry, s, -1e30)
    e = jnp.exp2(s - jnp.max(s, axis=0, keepdims=True))
    p = e * (1.0 / jnp.sum(e, axis=0, keepdims=True))
    dp = dot_t(v_all, diagonal(x[:, WIDE:LAT]))
    ds = (p * (dp - jnp.sum(p * dp, axis=0, keepdims=True))).astype(BF16).T
    o = dot(p.astype(BF16).T, v_all)
    dq = dot(ds, k_all) * scale
    dq_rope = dot(ds, r) * scale
    halves = (slice(0, TOK), slice(TOK, 2 * TOK))
    return [(o[h, c], dq[h, c], dq_rope[h, :]) for h, c in zip(halves, (slice(0, LANE), slice(LANE, WIDE)))]


def mega_kernel(scale, *refs):
    q_in, do_in, c_in, r_in, wk, wv, dkv = refs[:7]
    n_late = 3 * len(LATE)
    late = {u: refs[7 + 3 * i:10 + 3 * i] for i, u in enumerate(LATE)}
    late_sib = {u: refs[7 + n_late + 3 * i:10 + n_late + 3 * i] for i, u in enumerate(HANDED)}
    mega_body(scale, late, late_sib, q_in, do_in, c_in, r_in, wk, wv, dkv, *refs[7 + n_late + 3 * len(HANDED):])


def mega_body(scale, late, late_sib, q_in, do_in, c_in, r_in, wk, wv, dkv, wt_out, o_out, dq_out, dr_out, ct_out, dc_out,
              xbuf, cbuf, rbuf, ra, rb, wnat, wt, wt_own, kv, stage, kx, vs, qs, ps, dss, dr_acc, dr_land, pay, grow, osc, dqn, dqr, dos,
                c_send, c_recv, c_near, c_sib, x_send, x_recv, ici_send, ici_recv, sib_send, sib_recv,
                dr_send, dr_recv, load_sem, own_sem, wsem, xq_sem, wt_sem, st_sem):
    me = lax.axis_index("cp")
    core = me % 2
    chip = me // 2
    sib = flip(me, CORE)
    by_token = [pltpu.make_async_copy(src, dst, own_sem.at[n]) for n, (src, dst) in enumerate(((q_in, dq_out), (do_in, o_out)))]
    for cp in by_token:
        cp.start()
    bar = pltpu.get_barrier_semaphore()
    for m in range(1, N_DEV):
        pl.semaphore_signal(bar, inc=1, device_id=(flip(me, m),), device_id_type=MESH)
    pl.semaphore_wait(bar, N_DEV - 1)

    def remote(src, dst, ssem, rsem, to):
        return pltpu.make_async_remote_copy(src_ref=src, dst_ref=dst, send_sem=ssem, recv_sem=rsem,
                                            device_id=(to,), device_id_type=MESH)

    kept = ((c_in, cbuf, 0), (r_in, rbuf, 1))
    near_chips = (AX, AY, AZ)
    for src, buf, n in kept:
        for j, m in enumerate(near_chips):
            remote(src, buf.at[chip, core], c_send.at[n], c_near.at[n, j], flip(me, m)).start()
        remote(src, buf.at[chip, core], c_send.at[n], c_recv.at[n], flip(me, CHIPS[-1])).start()

    def pass_on():
        for _, buf, n in kept:
            for j, m in enumerate(near_chips):
                got = buf.at[flip(me, m) // 2, core]
                pltpu.make_async_copy(got, got, c_near.at[n, j]).wait()
                remote(got, got, c_send.at[n], c_recv.at[n], flip(me, near_chips[(j + 1) % 3])).start()

    own_c = [pltpu.make_async_copy(src, buf.at[chip, core], own_sem.at[2 + n]) for src, buf, n in kept]
    for cp in own_c:
        cp.start()

    def fetch_tile(tile, slot):
        return [pltpu.make_async_copy(w.at[:, pl.ds(pl.multiple_of(tile * SUB, SUB), SUB), :], wnat.at[slot, i], wsem.at[slot, i])
                for i, w in enumerate((wk, wv))]

    def own_tile(pp):
        return 4 * pp + place(me) // 4

    for pp in range(2):
        for cp in fetch_tile(own_tile(pp), pp):
            cp.start()
    for cp in by_token:
        cp.wait()

    def unpack_token(t, carry):
        rows = pl.ds(pl.multiple_of(t * PITCH, SUB), LANE)
        qt = dq_out[t].astype(F32)
        dqn[rows, :] = qt[:LANE, :].T
        dqr[rows, 0:ROPE] = qt[LANE:, :].T
        dos[rows, :] = o_out[t].astype(F32)
        return carry

    lax.fori_loop(0, TOK, unpack_token, 0, unroll=SUB)

    def pack_pair(p, carry):
        rope = []
        for a in range(2):
            rows = pl.ds(2 * p + a, TOK, stride=PITCH)
            pay[p, :, a * LANE:(a + 1) * LANE] = dqn[rows, :].astype(BF16)
            pay[p, :, (a + 2) * LANE:(a + 3) * LANE] = dos[rows, :].astype(BF16)
            rope.append(dqr[rows, :][:, :ROPE])
        pay[p, :, LAT:] = jnp.concatenate(rope, axis=-1).astype(BF16)
        return carry

    def to_owners(pp):
        for m in PEERS:
            to = flip(me, m)
            remote(pay.at[N_DEV * pp + place(to)], xbuf.at[pp, me], x_send, x_recv.at[pp], to).start()

    for pp in range(OWN):
        lax.fori_loop(N_DEV * pp, N_DEV * (pp + 1), pack_pair, 0, unroll=4)
        if pp == 1:
            pass_on()
        if pp:
            to_owners(pp - 1)

    dr_acc[...] = jnp.zeros_like(dr_acc)
    first = 2 * (place(me) % 4)
    for pp in range(OWN):
        for cp in fetch_tile(own_tile(pp), pp % 2):
            cp.wait()
        for i in range(2):
            wt[pp % 2, i] = jnp.transpose(wnat[pp % 2, i], (1, 0, 2))
            wt_own[pp, i] = wt[pp % 2, i, pl.ds(first, 2)]
        for cp in fetch_tile(own_tile(pp + 2), pp) if pp < 2 else fetch_tile(pp - 2, pp - 2):
            cp.start()
        if pp == 0:
            to_owners(OWN - 1)
    fwd = []
    for _, buf, n in kept:
        own_c[n].wait()
        arrived = buf.at[pl.ds(0, 4), 0]
        pltpu.make_async_copy(arrived, arrived, c_recv.at[n]).wait()
        fwd.append(remote(buf.at[:, core], buf.at[:, core], c_send.at[n], c_sib.at[n], sib))
        fwd[n].start()
    for cp in fwd:
        cp.wait_recv()

    def latent():
        return cbuf[...].reshape(SEQ, LAT)

    r_all = rbuf[...].reshape(SEQ, ROPE)
    ra[...] = jnp.concatenate([r_all, jnp.zeros_like(r_all)], axis=-1)
    rb[...] = jnp.concatenate([jnp.zeros_like(r_all), r_all], axis=-1)

    for pp in range(OWN):
        xbuf[pp, me] = pay[N_DEV * pp + place(me)]

    def block(mask, p, k):
        if p in LATE:
            return late[p][k].at[known(k, 2).index(mask)]
        return dkv.at[N_DEV * p + place(flip(me, mask)), pl.ds(2 * ROWS[k][0], 2 * ROWS[k][1]), :]

    def to_sibling(mask, p, k):
        if p == LATE[-1]:
            return
        b = block(mask, p, k)
        there = late_sib[p][k].at[known(k, 2).index(mask)] if p in LATE else b
        remote(b, there, sib_send, sib_recv.at[p], sib).start()

    def gather_stage(p, s):
        last = 2 if p in LATE else 3
        fresh = [[0] if s == 0 else [m + ORDERS[k][s - 1] for m in known(k, s - 1)] for k in range(3)]

        def arrive(k, m):
            b = block(m, p, k)
            pltpu.make_async_copy(b, b, ici_recv.at[p, k, m // 2]).wait()

        if s == last:
            for j in range(len(fresh[0])):
                for k in range(3):
                    arrive(k, fresh[k][j])
                    to_sibling(fresh[k][j], p, k)
            return
        for k in range(3):
            if s > 0:
                for m in fresh[k]:
                    arrive(k, m)
            d = ORDERS[k][s]
            for m in known(k, s):
                there = block(m + d, p, k) if p in LATE else block(m, p, k)
                remote(block(m, p, k), there, ici_send, ici_recv.at[p, k, (m + d) // 2], flip(me, d)).start()
        for k in range(3):
            for m in fresh[k]:
                to_sibling(m, p, k)

    def head_step(pp):
        got = xbuf.at[pp, pl.ds(0, N_DEV - 1)]
        pltpu.make_async_copy(got, got, x_recv.at[pp]).wait()
        x = xbuf[pp].reshape(SEQ, PACK)
        wkp = jnp.concatenate([wt_own[pp, 0, 0], wt_own[pp, 0, 1]], axis=-1)
        wvp = jnp.concatenate([wt_own[pp, 1, 0], wt_own[pp, 1, 1]], axis=-1)
        head_pair(scale, x, latent(), (ra[...], rb[...]), wkp, wvp, stage, dr_acc, kx, vs, qs, ps, dss)

        for p in range(OWN):
            @pl.when(pp == p)
            def _():
                cps = []
                for u, (pair, kind, n_kind) in enumerate(UNITS):
                    if pair != p:
                        continue
                    if u in LATE:
                        for k, (start, n) in enumerate(ROWS):
                            cps.append(pltpu.make_async_copy(
                                stage.at[pl.ds(2 * start + kind * n, n_kind * n), :], late[u][k].at[0], st_sem.at[3 * kind + k]))
                    else:
                        cps.append(pltpu.make_async_copy(stage, dkv.at[N_DEV * p + place(me)], st_sem.at[0]))
                for cp in cps:
                    cp.start()
                for cp in cps:
                    cp.wait()
                for u, unit in enumerate(UNITS):
                    if unit[0] == p:
                        gather_stage(u, 0)

    own_dr = pltpu.make_async_copy(dr_acc.at[pl.ds(pl.multiple_of(me * TOK, TOK), TOK), :], dr_out, load_sem.at[1])

    def share_rope():
        for m in range(1, N_DEV):
            to = flip(me, m)
            remote(dr_acc.at[pl.ds(pl.multiple_of(to * TOK, TOK), TOK), :], dr_land.at[me], dr_send, dr_recv, to).start()
        own_dr.start()

    def put_w(g, slot):
        return pltpu.make_async_copy(wt.at[slot], wt_out.at[:, pl.ds(pl.multiple_of(g * SUB, SUB), SUB)], wt_sem.at[slot])

    plan = {4: ((0, 1),), 5: ((1, 1),), 9: ((0, 2),), 10: ((1, 2),), 13: ((2, 1),), 15: tuple((u, 1) for u in LATE[1:])}

    def query_step(g, carry):
        slot = g % 2
        for cp in fetch_tile(g, slot):
            cp.wait()

        @pl.when((g > 0) & (g < 15))
        def _():
            for cp in fetch_tile(g + 1, 1 - slot):
                cp.start()

        @pl.when(g >= 2)
        def _():
            put_w(g - 2, slot).wait()

        for i in range(2):
            wt[slot, i] = jnp.transpose(wnat[slot, i], (1, 0, 2))
        put_w(g, slot).start()

        def project(j):
            c = latent()
            for i in range(2):
                kv[j % 2, i] = dot(c, jnp.concatenate([wt[slot, i, 2 * j], wt[slot, i, 2 * j + 1]], axis=-1)).astype(BF16)

        project(0)
        for j in range(4):
            if j < 3:
                project(j + 1)
            r = ra[...]
            res = query_pair(scale, me, pay[4 * g + j], kv[j % 2, 0], kv[j % 2, 1], r)
            for a in range(2):
                o, dq, dq_rope = res[a]
                osc[pl.ds(2 * j + a, TOK, stride=SUB), :] = o
                rows = pl.ds(g * SUB + 2 * j + a, TOK, stride=PITCH)
                dqn[rows, :] = dq
                dqr[rows, :] = dq_rope
        o_out[:, pl.ds(pl.multiple_of(g * SUB, SUB), SUB), :] = osc[...].reshape(TOK, SUB, LANE).astype(BF16)

        @pl.when(g < OWN)
        def _():
            head_step(g)

        @pl.when(g == OWN - 1)
        def _():
            share_rope()

        for when, events in plan.items():
            @pl.when(g == when)
            def _():
                for p, s in events:
                    gather_stage(p, s)
        return carry

    lax.fori_loop(0, 16, query_step, 0)

    def dq_token(t, carry):
        rows = pl.ds(pl.multiple_of(t * PITCH, SUB), LANE)
        dq_out[t, 0:LANE, :] = dqn[rows, :].T.astype(BF16)
        dq_out[t, LANE:192, :] = dqr[rows, :].T[0:ROPE, :].astype(BF16)
        return carry

    lax.fori_loop(0, TOK, dq_token, 0)
    ct_out[...] = latent().T
    put_w(14, 0).wait()
    put_w(15, 1).wait()
    for p in range(EARLY):
        gather_stage(p, 3)
    for p in range(EARLY):
        got = dkv.at[pl.ds(N_DEV * p, SUB)]
        pltpu.make_async_copy(got, got, sib_recv.at[p]).wait()

    def rows_of(t, slot):
        cps = [pltpu.make_async_copy(wt_out.at[:, pl.ds(pl.multiple_of(t * SUB, SUB), SUB)], wt.at[slot], wt_sem.at[slot])]
        for n in range(4):
            for i in range(2):
                at = pl.ds(own_sixteen(me, n, i), N_DEV)
                cps.append(pltpu.make_async_copy(dkv.at[pl.ds(4 * t, 4), at, :],
                                                 grow.at[slot, i, :, pl.ds(N_DEV * n, N_DEV), :], xq_sem.at[slot, 4 * i + n]))
        return cps

    for cp in rows_of(0, 0):
        cp.start()
    dc_out[...] = jnp.zeros_like(dc_out)

    def dc_step(t, carry):
        slot = t % 2
        for cp in rows_of(t, slot):
            cp.wait()

        @pl.when(t < SUB - 1)
        def _():
            for cp in rows_of(t + 1, 1 - slot):
                cp.start()

        for i in range(2):
            for j in range(4):
                w = jnp.concatenate([wt[slot, i, 2 * j], wt[slot, i, 2 * j + 1]], axis=-1)
                dc_out[...] += dot_t(grow[slot, i, j], w)
        return carry

    lax.fori_loop(0, SUB, dc_step, 0)
    for p in LATE:
        gather_stage(p, 2)

    own_dr.wait()
    got = dr_land.at[pl.ds(0, N_DEV - 1)]
    pltpu.make_async_copy(got, got, dr_recv).wait()
    total = dr_out[...]
    for m in range(1, N_DEV):
        total = total + dr_land[flip(me, m)]
    dr_out[...] = total

    pltpu.make_async_copy(got, got, dr_send).wait()
    got = xbuf.at[:, pl.ds(0, N_DEV - 1)]
    pltpu.make_async_copy(got, got, x_send).wait()
    for _, buf, n in kept:
        for arrived in (buf.at[pl.ds(0, 7), 0], buf.at[:, 0]):
            pltpu.make_async_copy(arrived, arrived, c_send.at[n]).wait()
    sent = dkv.at[pl.ds(0, 20)]
    pltpu.make_async_copy(sent, sent, ici_send).wait()
    sent = dkv.at[pl.ds(0, 20)]
    pltpu.make_async_copy(sent, sent, sib_send).wait()
    for p in HANDED:
        got = dkv.at[pl.ds(0, 2 * UNITS[p][2])]
        pltpu.make_async_copy(got, got, sib_recv.at[p]).wait()


def mega(scale, q_t, d_out, latent, key_rope, wk, wv):
    any_spec = pl.BlockSpec(memory_space=pl.ANY)
    vmem = pl.BlockSpec(memory_space=pltpu.VMEM)
    dma = pltpu.SemaphoreType.DMA
    return pl.pallas_call(
        functools.partial(mega_kernel, scale),
        in_specs=[any_spec] * 6,
        out_specs=[any_spec] * (2 + 3 * len(LATE) + 3 * len(HANDED)) + [vmem] * 5,
        out_shape=[
            jax.ShapeDtypeStruct((32, BOTH, WIDE), BF16),
            *[jax.ShapeDtypeStruct((4, UNITS[u][2] * n, WIDE), BF16) for u in (*LATE, *HANDED) for _, n in ROWS],
            jax.ShapeDtypeStruct((2, LANE, LAT, LANE), BF16),
            jax.ShapeDtypeStruct((TOK, LANE, LANE), BF16),
            jax.ShapeDtypeStruct((TOK, 192, LANE), BF16),
            jax.ShapeDtypeStruct((TOK, LANE), F32),
            jax.ShapeDtypeStruct((LAT, SEQ), BF16),
            jax.ShapeDtypeStruct((TOK, LAT), F32),
        ],
        scratch_shapes=[
            pltpu.VMEM((OWN, N_DEV, TOK, PACK), BF16),
            pltpu.VMEM((SUB, 2, TOK, LAT), BF16), pltpu.VMEM((SUB, 2, TOK, ROPE), BF16),
            pltpu.VMEM((SEQ, LANE), BF16), pltpu.VMEM((SEQ, LANE), BF16),
            pltpu.VMEM((2, 2, LAT, SUB, LANE), BF16),
            pltpu.VMEM((2, 2, SUB, LAT, LANE), BF16),
            pltpu.VMEM((OWN, 2, 2, LAT, LANE), BF16),
            pltpu.VMEM((2, 2, SEQ, WIDE), BF16),
            pltpu.VMEM((BOTH, WIDE), BF16),
            pltpu.VMEM((SEQ, WIDE), BF16), pltpu.VMEM((SEQ, WIDE), BF16), pltpu.VMEM((SEQ, WIDE), BF16),
            pltpu.VMEM((SEQ, SEQ), BF16), pltpu.VMEM((SEQ, SEQ), BF16),
            pltpu.VMEM((SEQ, LANE), F32),
            pltpu.VMEM((N_DEV, TOK, LANE), F32),
            pltpu.VMEM((PAIRS, TOK, PACK), BF16),
            pltpu.VMEM((2, 2, 4, TOK, WIDE), BF16),
            pltpu.VMEM((TOK * SUB, LANE), F32),
            *[pltpu.VMEM((TOK * PITCH, LANE), F32)] * 3,
            dma((2,)), dma((2,)), dma((2, 3)), dma((2,)), dma, dma((OWN,)), dma, dma((len(UNITS), 3, SUB)), dma, dma((len(UNITS),)),
            dma, dma, dma((2,)), dma((4,)), dma((2, 2)), dma((2, SUB)), dma((2,)), dma((6,)),
        ],
        compiler_params=pltpu.CompilerParams(collective_id=0, has_side_effects=True, vmem_limit_bytes=VMEM_ALL),
        cost_estimate=pl.CostEstimate(flops=100_000_000_000, bytes_accessed=200_000_000, transcendentals=0),
        name="mega",
    )(q_t, d_out, latent, key_rope, wk, wv)


def weight_kernel(dkv_ref, ct_ref, dwk_ref, dwv_ref):
    for which, out_ref in enumerate((dwk_ref, dwv_ref)):
        flat = out_ref.reshape(LAT * SUB, LANE)
        for p in range(4):
            g = jnp.concatenate([dkv_ref[p, at:at + n, :] for _, n, at in segments(which, 0, SEQ)], axis=0)
            for m in range(2):
                res = dot(ct_ref[m * WIDE:(m + 1) * WIDE, :], g)
                for a in range(2):
                    flat[pl.ds(m * BOTH + 2 * p + a, WIDE, stride=SUB), :] = res[:, a * LANE:(a + 1) * LANE]


def weight_part(dkv, ct):
    out_block = pl.BlockSpec((LAT, SUB, LANE), lambda g: (0, g, 0))
    return pl.pallas_call(
        weight_kernel,
        grid=(SUB,),
        in_specs=[
            pl.BlockSpec((4, BOTH, WIDE), lambda g: (g, 0, 0)),
            pl.BlockSpec((LAT, SEQ), lambda g: (0, 0)),
        ],
        out_specs=[out_block, out_block],
        out_shape=[jax.ShapeDtypeStruct((LAT, LANE, LANE), F32)] * 2,
        compiler_params=pltpu.CompilerParams(vmem_limit_bytes=VMEM_ALL),
        cost_estimate=pl.CostEstimate(flops=18_000_000_000, bytes_accessed=70_000_000, transcendentals=0),
        name="weight_part",
    )(dkv, ct)


def late_kernel(unit, other, with_rows, *refs):
    pair, kind, n_kind = unit
    near, far = refs[0:3], refs[3:6]
    ct_in, wt, dc_in = refs[6:9]
    refs = refs[9 + n_kind:]
    rows_in, refs = (refs[:2], refs[2:]) if with_rows else ((), refs)
    grads, dc_out, refs = refs[:n_kind], refs[n_kind], refs[n_kind + 1:]
    rows_out, refs = (refs[:2], refs[2:]) if with_rows else ((), refs)
    ct, dc_buf, dc_last, gbuf, wbuf, obuf, ct_sem, gsem, wsem, osem = refs[:10]
    refs = refs[10:]
    me = lax.axis_index("cp")
    src = flip(me, CORE) if other else me
    own = pl.ds(pl.multiple_of(me * TOK, TOK), TOK)
    tiles = [4 * pair + place(flip(src, AZ * b)) // 4 for b in range(2)]
    load_ct = pltpu.make_async_copy(ct_in, ct, ct_sem.at[0])
    load_dc = pltpu.make_async_copy(dc_in, dc_buf, ct_sem.at[1])

    def fetch(n):
        b, i = n // n_kind, n % n_kind
        for j in range(4):
            mask = AZ * b + 2 * j
            for k, (start, n_row) in enumerate(ROWS):
                d = ORDERS[k][2]
                ref, m = (far[k], mask - d) if mask & d else (near[k], mask)
                pltpu.make_async_copy(ref.at[known(k, 2).index(m), pl.ds(i * n_row, n_row)],
                                      gbuf.at[b, i, j, pl.ds(start, n_row), :], gsem.at[b, i]).start()

    def fetch_w(n):
        b, i = n // n_kind, n % n_kind
        pltpu.make_async_copy(wt.at[kind + i, pl.ds(pl.multiple_of(tiles[b] * SUB, SUB), SUB)], wbuf.at[b, i], wsem.at[b, i]).start()

    fetch(0)
    load_ct.start()
    load_dc.start()
    fetch(1)
    moves = []
    for n in range(len(rows_in)):
        moves.append((pltpu.make_async_copy(rows_in[n], refs[n], refs[-1].at[n]),
                      pltpu.make_async_copy(refs[n], rows_out[n], refs[-1].at[n])))
        moves[-1][0].start()

    def store(b, i, tile):
        where = grads[i].at[:, pl.ds(pl.multiple_of(tile * SUB, SUB), SUB), :]
        return pltpu.make_async_copy(obuf.at[b, i].reshape(LAT, SUB, LANE), where, osem.at[b, i])

    x, y = (src // AX) % 2, (src // AY) % 2
    load_ct.wait()
    load_dc.wait()

    def half_tile(n, carried):
        b, i = n // n_kind, n % n_kind
        tile = tiles[0] + b * (tiles[1] - tiles[0])
        slots = []
        for j in range(4):
            dx, dy = j % 2, j // 2
            slots.append(2 * (2 * (y + dy - 2 * y * dy) + x + dx - 2 * x * dx))
        pltpu.make_async_copy(gbuf.at[b, i], gbuf.at[b, i], gsem.at[b, i]).wait()
        for now in range(2 * n_kind):
            @pl.when(n == now)
            def _():
                if now + 2 < 2 * n_kind:
                    fetch(now + 2)
                fetch_w(now)
        for j in range(4):
            for m in range(2):
                res = dot(ct[m * WIDE:(m + 1) * WIDE, :], gbuf[b, i, j])
                for a in range(2):
                    obuf[b, i, pl.ds(m * BOTH + slots[j] + a, WIDE, stride=SUB), :] = res[:, a * LANE:(a + 1) * LANE]
        for which in range(n_kind):
            @pl.when(i == which)
            def _():
                store(b, which, tile).start()
        return carried

    lax.fori_loop(0, 2 * n_kind, half_tile, 0)
    dc = dc_buf[...]
    for b in range(2):
        for i in range(n_kind):
            pltpu.make_async_copy(wbuf.at[b, i], wbuf.at[b, i], wsem.at[b, i]).wait()
            for j in range(4):
                dx, dy = j % 2, j // 2
                slot = 2 * (2 * (y + dy - 2 * y * dy) + x + dx - 2 * x * dx)
                dc += dot_t(gbuf[b, i, j, own, :], jnp.concatenate([wbuf[b, i, slot], wbuf[b, i, slot + 1]], axis=-1))
    dc_buf[...] = dc
    dc_last[...] = dc_buf[...].astype(dc_last.dtype)
    put_dc = pltpu.make_async_copy(dc_last, dc_out, ct_sem.at[0])
    put_dc.start()
    for load, put in moves:
        load.wait()
        put.start()
    for load, put in moves:
        put.wait()
    for b in range(2):
        for i in range(n_kind):
            store(b, i, tiles[b]).wait()
    put_dc.wait()


def late_part(unit, other, near, far, ct, wt, dc, grads, dc_type, rows=()):
    n_kind = unit[2]
    any_spec = pl.BlockSpec(memory_space=pl.ANY)
    dma = pltpu.SemaphoreType.DMA
    like = lambda arrays: [jax.ShapeDtypeStruct(r.shape, r.dtype) for r in arrays]
    res = pl.pallas_call(
        functools.partial(late_kernel, unit, other, bool(rows)),
        in_specs=[any_spec] * (9 + n_kind + len(rows)),
        out_specs=[any_spec] * (n_kind + 1 + len(rows)),
        out_shape=like(grads) + [jax.ShapeDtypeStruct(dc.shape, dc_type)] + like(rows),
        scratch_shapes=[
            pltpu.VMEM((LAT, SEQ), BF16), pltpu.VMEM(dc.shape, F32), pltpu.VMEM(dc.shape, dc_type),
            pltpu.VMEM((2, n_kind, 4, SEQ, WIDE), BF16),
            pltpu.VMEM((2, n_kind, SUB, LAT, LANE), BF16),
            pltpu.VMEM((2, n_kind, 2 * BOTH, LANE), F32),
            dma((2,)), dma((2, n_kind)), dma((2, n_kind)), dma((2, n_kind)),
            *([pltpu.VMEM(r.shape, r.dtype) for r in rows] + [dma((2,))] if rows else []),
        ],
        input_output_aliases={9 + n: n for n in range(n_kind)},
        compiler_params=pltpu.CompilerParams(vmem_limit_bytes=VMEM_ALL),
        cost_estimate=pl.CostEstimate(flops=2_200_000_000 * n_kind, bytes_accessed=10_000_000 * n_kind, transcendentals=0),
        name="late_part",
    )(*near, *far, ct, wt, dc, *grads, *rows)
    return res[:n_kind], res[n_kind], res[n_kind + 1:]


def solution(mesh):
    seq_spec = P("cp")

    def local_step(queries, latent, key_rope, w_uk, w_uv, d_out):
        scale = 1.0 / math.sqrt(queries.shape[-1])
        dkv, *late, wt, o, dq, dr, ct, dc = mega(scale, queries.transpose(0, 2, 1), d_out, latent, key_rope, w_uk, w_uv)
        mine = {u: late[3 * i:3 * i + 3] for i, u in enumerate(LATE)}
        sibs = {u: late[3 * (i + len(LATE)):][:3] for i, u in enumerate(HANDED)}

        def swap(a, d):
            return lax.ppermute(a, "cp", [(i, i ^ d) for i in range(N_DEV)])

        far = {}
        for u in LATE:
            far[u] = [swap(a, ORDERS[k][2]) for k, a in enumerate(mine[u])]
        sibs[LATE[-1]] = [swap(a, CORE) for a in mine[LATE[-1]]]
        grads = list(weight_part(dkv, ct))
        for u in LATE:
            got, grads, dc = lax.optimization_barrier((far[u], grads, dc))
            got_sib = [swap(a, CORE) for a in got]
            _, kind, n_kind = UNITS[u]
            for other, near, here in ((False, mine[u], got), (True, sibs[u], got_sib)):
                rows = (o, dq) if other and u == EARLY else ()
                grads[kind:kind + n_kind], dc, rows = late_part(
                    UNITS[u], other, near, here, ct, wt, dc, grads[kind:kind + n_kind],
                    BF16 if other and u == LATE[-1] else F32, rows)
                if rows:
                    o, dq = rows
        dwk, dwv = grads
        d_key_rope = (dr[:, :ROPE] + dr[:, ROPE:]).astype(BF16)
        return o, dq.transpose(0, 2, 1), dc, d_key_rope, dwk, dwv

    return jax.shard_map(local_step, mesh=mesh,
                         in_specs=(seq_spec, seq_spec, seq_spec, P(), P(), seq_spec),
                         out_specs=(seq_spec, seq_spec, seq_spec, seq_spec, P(), P()),
                         check_vma=False)
```
